32 devices in a mesh: tm: 8 (over y, x, core), space: 4 (over z).
Axes of the slice: x: 2, y: 2, z: 4, core: 2. Of those that a mesh axis runs over, the one named last changes fastest.
Arguments:
- state: float32 [16, 32, 64, 256], P('tm', 'space'), may hold values from -1.5 to 1.5
- initial: float32 [32, 64, 256], P('space'), may hold values from -1.5 to 1.5
Outputs:
- updated: float32 [16, 32, 64, 256], P('tm', 'space')
- residual: float32 [16, 32, 64, 256], P('tm', 'space')
The draws below stay inside these ranges and needn't reach their ends.
All inputs are finite; a program needn't handle non-finite values.
Results may differ from the reference program's by a relative error of at most 0.0003.
Values sent between devices are 32-bit elements; how exact they have to be, the bound alone decides.
No kernel may reach another device: no remote copies, remote signals or barrier semaphores. Data moves between devices by JAX's collectives and lax.ppermute only.
A program may use at most 64 MiB of HBM per device.

```python
import math
import jax
import jax.numpy as jnp
from jax import lax

NY = 64
NZ = 256
SWEEPS = 6
STEPS = 16
NX = 32


def draw_state(key, part):
    shape = (STEPS, NX, NY, NZ)
    return jax.random.uniform(key, shape, jnp.float32, -1.5, 1.5)


def block_levels(key, dims, split, low, largest):
    loudness, own = 1.0, jax.random.fold_in(key, 6)
    for axis_at, shards_of in split:
        steps = jnp.exp(jax.random.uniform(jax.random.fold_in(own, axis_at), (shards_of,), jnp.float32, low / len(split), largest / len(split)))
        loudness = loudness * jnp.repeat(steps, dims[axis_at] // shards_of).reshape([-1 if axis == axis_at else 1 for axis in range(len(dims))])
    return loudness


def setup_inputs(seed: int = 0) -> dict:
    seeds = jax.random.split(jax.random.key(seed), 3)
    state = draw_state(jax.random.fold_in(seeds[2], 71), 0)
    initial = jnp.clip(jax.random.uniform(seeds[1], (NX, NY, NZ), jnp.float32, -1.5, 1.5) * block_levels(seeds[1], (NX, NY, NZ), ((0, 4),), -0.4, 0.0), -1.5, 1.5)
    return dict(state=state, initial=initial)


alpha_value = 0.1
time_step = 0.1
couple_first = 0.4
couple_cross = 0.05
reaction_shift = 0.1
relaxation = 0.9


def first_sum(field):
    return jnp.roll(field, 1, -3) + jnp.roll(field, -1, -3)


def cross_sum(field):
    return (jnp.roll(field, 1, -2) + jnp.roll(field, -1, -2)
            + jnp.roll(field, 1, -1) + jnp.roll(field, -1, -1))


def phases(lefts, rights, horizon):
    products = (lefts[:, None] * rights[None, :]) % horizon
    return (2.0 * math.pi / horizon) * products.astype(jnp.float32)


def scales(horizon):
    counter = jnp.arange(horizon)
    return jnp.power(alpha_value, counter.astype(jnp.float32) / horizon)


def mode_diagonal(modes, horizon):
    root_alpha = alpha_value ** (1.0 / horizon)
    angles = (2.0 * math.pi / horizon) * modes.astype(jnp.float32)
    diag_real = 1.0 - root_alpha * jnp.cos(angles) + reaction_shift + 2.0 * couple_first + 4.0 * couple_cross
    diag_imag = root_alpha * jnp.sin(angles)
    return diag_real, diag_imag


def reference(state, initial):
    horizon = state.shape[0]
    before = jnp.concatenate([initial[None], state[:-1]], axis=0)
    laplace = couple_first * (first_sum(state) - 2.0 * state) + couple_cross * (cross_sum(state) - 4.0 * state)
    residual = before - state + laplace + time_step * (state - state * state * state)
    counter = jnp.arange(horizon)
    angles = phases(counter, counter, horizon)
    weight = scales(horizon)
    fore_cos = jnp.cos(angles) * weight[None, :]
    fore_sin = -jnp.sin(angles) * weight[None, :]
    back_cos = jnp.cos(angles).T / (horizon * weight[:, None])
    back_sin = -jnp.sin(angles).T / (horizon * weight[:, None])
    highest = lax.Precision.HIGHEST
    spec_real = jnp.einsum('kn,nxyz->kxyz', fore_cos, residual, precision=highest)
    spec_imag = jnp.einsum('kn,nxyz->kxyz', fore_sin, residual, precision=highest)
    diag_real, diag_imag = mode_diagonal(counter, horizon)
    magnitude = diag_real * diag_real + diag_imag * diag_imag
    inv_real = diag_real / magnitude
    inv_imag = -diag_imag / magnitude

    def solve_mode(operands):
        source_real, source_imag, real_part, imag_part = operands
        solved_real = relaxation * (real_part * source_real - imag_part * source_imag)
        solved_imag = relaxation * (real_part * source_imag + imag_part * source_real)
        for sweep_index in range(SWEEPS - 1):
            total_real = source_real + (couple_first * first_sum(solved_real) + couple_cross * cross_sum(solved_real))
            total_imag = source_imag + (couple_first * first_sum(solved_imag) + couple_cross * cross_sum(solved_imag))
            solved_real, solved_imag = (
                (1.0 - relaxation) * solved_real + relaxation * (real_part * total_real - imag_part * total_imag),
                (1.0 - relaxation) * solved_imag + relaxation * (imag_part * total_real + real_part * total_imag))
        return solved_real, solved_imag

    solved_real, solved_imag = lax.map(solve_mode, (spec_real, spec_imag, inv_real, inv_imag))
    delta = (jnp.einsum('nk,kxyz->nxyz', back_cos, solved_real, precision=highest)
             + jnp.einsum('nk,kxyz->nxyz', back_sin, solved_imag, precision=highest))
    return state + delta, residual
```

```python
import functools
import math

import jax
import jax.numpy as jnp
import numpy as np
from jax import lax
from jax.experimental import pallas as pl
from jax.experimental.pallas import tpu as pltpu
from jax.sharding import PartitionSpec as P

SWEEPS = 6
EARLY = 3

alpha_value = 0.1
time_step = 0.1
couple_first = 0.4
couple_cross = 0.05
reaction_shift = 0.1
relaxation = 0.9

PAD = 8
VMEM_LIMIT = 60 * 1024 * 1024


def ring(axis, step):
    count = lax.axis_size(axis)
    return [(i, (i + step) % count) for i in range(count)]


def hop(block, step):
    return lax.ppermute(block, "space", ring("space", step))


def tile_of(low, high):
    return jnp.concatenate([low, high], axis=0).T


def windows(tile, count):
    third = tile.shape[0]
    size = third // count
    padded = jnp.concatenate([tile[third - PAD :], tile, tile[:PAD]], axis=0)
    return [padded[b * size : b * size + size + 2 * PAD] for b in range(count)]


def pack_own(position, state, initial, out, first, stage):
    count, steps, pairs, rows, lanes = out.shape
    width = state.shape[1]
    third = state.shape[3]
    size = third // count
    for pair in range(pairs):
        tile = tile_of(initial[pair], initial[width - 1 - pair])
        stage[:PAD] = tile[third - PAD :]
        stage[PAD : PAD + third] = tile
        stage[PAD + third :] = tile[:PAD]
        first[pair] = stage[pl.ds(pl.multiple_of(position[0] * size, 8), rows), :]
        for step in range(steps):
            tile = tile_of(state[step, pair], state[step, width - 1 - pair])
            for b, window in enumerate(windows(tile, count)):
                out[b, step, pair] = window


def pack_early(lower, upper, out):
    count, steps, depth, rows, lanes = out.shape
    for step in range(steps):
        for j in range(depth):
            tile = tile_of(lower[step, j], upper[step, depth - 1 - j])
            for b, window in enumerate(windows(tile, count)):
                out[b, step, j] = window


def swap(tile):
    return pltpu.roll(tile, tile.shape[-1] // 2, tile.ndim - 1)


def low_mask(tile):
    lanes = tile.shape[-1]
    return lax.broadcasted_iota(jnp.int32, tile.shape, tile.ndim - 1) < lanes // 2


def pack_late(skip, own, up, down):
    half, late, rows, lanes = up.shape
    pairs = own.shape[1]
    width = 2 * pairs
    depth = SWEEPS

    def step(t, carry):
        for j in range(late):
            a = depth - j
            for out, layer in ((up, width - a), (down, a - 1)):
                pair, in_low = (layer, True) if layer < pairs else (width - 1 - layer, False)
                early = own[t, pair, skip : skip + rows]
                later = own[t + half, pair, skip : skip + rows]
                if in_low:
                    out[t, j] = jnp.where(low_mask(early), early, swap(later))
                else:
                    out[t, j] = jnp.where(low_mask(early), swap(early), later)
        return carry

    lax.fori_loop(0, half, step, 0)


def real_forward(values):
    count = len(values)
    if count == 1:
        return [(values[0], None)]
    if count == 2:
        return [(values[0] + values[1], None), (values[0] - values[1], None)]
    even = real_forward(values[0::2])
    odd = real_forward(values[1::2])
    half = count // 2
    result = [None] * (half + 1)
    for k in range(count // 4 + 1):
        even_real, even_imag = even[k]
        odd_real, odd_imag = odd[k]
        if k == 0:
            result[0] = (even_real + odd_real, None)
            result[half] = (even_real - odd_real, None)
        elif 4 * k == count:
            result[k] = (even_real, -odd_real)
        else:
            cos, sin = math.cos(2 * math.pi * k / count), math.sin(2 * math.pi * k / count)
            if odd_imag is None:
                turned_real, turned_imag = cos * odd_real, -sin * odd_real
            else:
                turned_real = cos * odd_real + sin * odd_imag
                turned_imag = cos * odd_imag - sin * odd_real
            if even_imag is None:
                result[k] = (even_real + turned_real, turned_imag)
                result[half - k] = (even_real - turned_real, turned_imag)
            else:
                result[k] = (even_real + turned_real, even_imag + turned_imag)
                result[half - k] = (even_real - turned_real, turned_imag - even_imag)
    return result


def real_inverse(modes):
    half = len(modes) - 1
    count = 2 * half
    if count == 2:
        return [modes[0][0] + modes[1][0], modes[0][0] - modes[1][0]]
    even, odd = [], []
    for k in range(count // 4 + 1):
        real, imag = modes[k]
        other_real, other_imag = modes[half - k]
        if k == 0:
            even.append((real + other_real, None))
            odd.append((real - other_real, None))
        elif 4 * k == count:
            even.append((2.0 * real, None))
            odd.append((-2.0 * imag, None))
        else:
            cos, sin = math.cos(2 * math.pi * k / count), math.sin(2 * math.pi * k / count)
            even.append((real + other_real, imag - other_imag))
            minus_real, minus_imag = real - other_real, imag + other_imag
            odd.append((cos * minus_real - sin * minus_imag, sin * minus_real + cos * minus_imag))
    result = [None] * count
    result[0::2] = real_inverse(even)
    result[1::2] = real_inverse(odd)
    return result


def mode_inverses(horizon):
    rho = alpha_value ** (1.0 / horizon)
    angles = 2.0 * math.pi * np.arange(horizon // 2 + 1) / horizon
    shift = (
        1.0 + reaction_shift + 2.0 * couple_first + 4.0 * couple_cross - rho * np.cos(angles)
    ) + 1j * rho * np.sin(angles)
    return 1.0 / shift


def sweep_table(horizon):
    inverse = relaxation * mode_inverses(horizon)
    rows = [(inverse[0].real, 0.0, 0.0, inverse[-1].real)]
    rows += [(v.real, -v.imag, v.imag, v.real) for v in inverse[1:-1]]
    return couple_cross * np.array(rows, np.float32)


def second_sum(tile):
    lanes = tile.shape[-1]
    axis = tile.ndim - 1
    place = lax.broadcasted_iota(jnp.int32, tile.shape, axis) % (lanes // 2)
    before = jnp.where(
        place == 0, pltpu.roll(tile, lanes // 2 + 1, axis), pltpu.roll(tile, 1, axis)
    )
    after = jnp.where(
        place == lanes // 2 - 1,
        pltpu.roll(tile, lanes // 2 - 1, axis),
        pltpu.roll(tile, lanes - 1, axis),
    )
    return before + after


def solve(skip, table, up, down, first, first_low, first_high, own, early, out, state, base, ping, pong, sems):
    horizon, pairs = own.shape[:2]
    taken = early.shape[1]
    depth = SWEEPS
    late = depth - taken
    rows = own.shape[2]
    post_rows = up.shape[2]
    block = rows - 2 * PAD
    last = depth + pairs - 1
    half = horizon // 2
    at = PAD
    copies = [
        pltpu.make_async_copy(
            own, state.at[pl.ds(1, horizon), pl.ds(depth, pairs), pl.ds(at, rows)], sems.at[0]
        ),
        pltpu.make_async_copy(
            early, state.at[pl.ds(1, horizon), pl.ds(late, taken), pl.ds(at, rows)], sems.at[1]
        ),
    ]
    for copy in copies:
        copy.start()

    for i in range(pairs):
        state[0, depth + i, at : at + rows] = first[i]
    for a in range(1, depth):
        if a <= pairs:
            low, high = first_low[a - 1], first_high[a - 1]
            tile = swap(jnp.where(low_mask(low), high, low))
        else:
            low, high = first_low[2 * pairs - a], first_high[2 * pairs - a]
            tile = jnp.where(low_mask(low), low, high)
        state[0, depth - a, at : at + rows] = tile

    def place(t, carry):
        for j in range(late):
            low, high = up[t, j], down[t, j]
            mask = low_mask(low)
            here = slice(at + skip, at + skip + post_rows)
            state[1 + t, j, here] = jnp.where(mask, low, swap(high))
            state[1 + half + t, j, here] = jnp.where(mask, swap(low), high)
        return carry

    lax.fori_loop(0, half, place, 0)
    for copy in copies:
        copy.wait()

    def mirror(t, carry):
        state[t, last + 1, at : at + rows] = swap(state[t, last, at : at + rows])
        return carry

    lax.fori_loop(0, horizon + 1, mirror, 0)

    def weigh(t, carry):
        for x in range(1, last + 1):
            s = state[t + 1, x, at : at + rows]
            along = state[t + 1, x - 1, at : at + rows] + state[t + 1, x + 1, at : at + rows]
            across = (
                state[t + 1, x, at - 1 : at + rows - 1]
                + state[t + 1, x, at + 1 : at + rows + 1]
                + second_sum(s)
            )
            centre = time_step - 1.0 - 2.0 * couple_first - 4.0 * couple_cross
            ping[t, x, at : at + rows] = (
                (state[t, x, at : at + rows] + couple_first * along)
                + (couple_cross * across + s * (centre - time_step * (s * s)))
            )
        return carry

    lax.fori_loop(0, horizon, weigh, 0)

    inverses = mode_inverses(horizon)
    weights = [alpha_value ** (n / horizon) for n in range(horizon)]
    tiles = rows // 8

    def transform(index, carry):
        x = 1 + index // tiles
        r = pl.ds(pl.multiple_of(at + (index % tiles) * 8, 8), 8)
        spectrum = real_forward([weights[n] * ping[n, x, r, :] for n in range(horizon)])
        for k, (real, imag) in enumerate(spectrum):
            c = relaxation * inverses[k]
            if k == 0:
                base[0, x, r, :] = float(c.real) * real
            elif k == half:
                base[half, x, r, :] = float(c.real) * real
            else:
                base[k, x, r, :] = float(c.real) * real - float(c.imag) * imag
                base[half + k, x, r, :] = float(c.imag) * real + float(c.real) * imag
        return carry

    lax.fori_loop(0, last * tiles, transform, 0)

    def mirror_base(k, carry):
        base[k, last + 1, at : at + rows] = swap(base[k, last, at : at + rows])
        return carry

    lax.fori_loop(0, horizon, mirror_base, 0)

    def sweep(number, source, target):
        def pair(k, carry):
            a, b, c, d = [table[k, i] for i in range(4)]
            for x in range(number + 1, last + 1):
                near = []
                for m in (k, half + k):
                    v = source[m, x, at : at + rows]
                    along = source[m, x - 1, at : at + rows] + source[m, x + 1, at : at + rows]
                    across = (
                        source[m, x, at - 1 : at + rows - 1]
                        + source[m, x, at + 1 : at + rows + 1]
                        + second_sum(v)
                    )
                    near.append(
                        (
                            base[m, x, at : at + rows] + (1.0 - relaxation) * v,
                            (couple_first / couple_cross) * along + across,
                        )
                    )
                (rest_real, near_real), (rest_imag, near_imag) = near
                real = rest_real + (a * near_real + b * near_imag)
                imag = rest_imag + (c * near_real + d * near_imag)
                target[k, x, at : at + rows] = real
                target[half + k, x, at : at + rows] = imag
                if x == last:
                    target[k, last + 1, at : at + rows] = swap(real)
                    target[half + k, last + 1, at : at + rows] = swap(imag)
            return carry

        lax.fori_loop(0, half, pair, 0)

    source = base
    for number in range(1, SWEEPS):
        target = ping if number % 2 else pong
        sweep(number, source, target)
        source = target

    kept = block // 8

    def restore(index, carry):
        i = index // kept
        r = pl.ds(pl.multiple_of(at + PAD + (index % kept) * 8, 8), 8)
        modes = [(source[0, depth + i, r, :], None)]
        modes += [
            (source[k, depth + i, r, :], source[half + k, depth + i, r, :]) for k in range(1, half)
        ]
        modes += [(source[half, depth + i, r, :], None)]
        place_at = pl.ds(pl.multiple_of((index % kept) * 8, 8), 8)
        for n, value in enumerate(real_inverse(modes)):
            out[n, i, place_at, :] = (1.0 / (horizon * weights[n])) * value
        return carry

    lax.fori_loop(0, pairs * kept, restore, 0)


def finish(state, pieces, updated):
    count, steps, pairs, size, lanes = pieces.shape
    width = 2 * pairs
    second = lanes // 2
    for step in range(steps):
        for pair in range(pairs):
            tile = jnp.concatenate([pieces[b, step, pair] for b in range(count)], axis=0).T
            updated[step, pair] = state[step, pair] + tile[:second]
            updated[step, width - 1 - pair] = state[step, width - 1 - pair] + tile[second:]


def residual_of(state, carried, low, high, out):
    steps, width = state.shape[:2]
    for step in range(steps):
        for layer in range(width):
            s = state[step, layer]
            below = low[step] if layer == 0 else state[step, layer - 1]
            above = high[step] if layer == width - 1 else state[step, layer + 1]
            before = carried[layer] if step == 0 else state[step - 1, layer]
            across = (
                pltpu.roll(s, 1, 0)
                + pltpu.roll(s, s.shape[0] - 1, 0)
                + pltpu.roll(s, 1, 1)
                + pltpu.roll(s, s.shape[1] - 1, 1)
            )
            centre = time_step - 1.0 - 2.0 * couple_first - 4.0 * couple_cross
            out[step, layer] = (
                (before + couple_first * (below + above))
                + (couple_cross * across + s * (centre - time_step * (s * s)))
            )


def vmem(count):
    return [pl.BlockSpec(memory_space=pltpu.VMEM)] * count


def shape_of(*dims):
    return jax.ShapeDtypeStruct(dims, jnp.float32)


def params():
    return pltpu.CompilerParams(vmem_limit_bytes=VMEM_LIMIT)


def cost(flops, bytes_accessed):
    return pl.CostEstimate(flops=int(flops), bytes_accessed=int(bytes_accessed), transcendentals=0)


def body(state, initial):
    steps, width, second, third = state.shape
    count = lax.axis_size("tm")
    horizon = steps * count
    position = lax.axis_index("tm")
    depth, taken = SWEEPS, EARLY
    late = depth - taken
    pairs = width // 2
    size = third // count
    rows = size + 2 * PAD
    lanes = 2 * second
    skip = 4
    post_rows = rows - 2 * skip

    lower = hop(state[:, width - taken :], 1)
    upper = hop(state[:, :taken], -1)

    sent, first = pl.pallas_call(
        pack_own,
        out_shape=(shape_of(count, steps, pairs, rows, lanes), shape_of(pairs, rows, lanes)),
        in_specs=[pl.BlockSpec(memory_space=pltpu.SMEM)] + vmem(2),
        out_specs=vmem(2),
        scratch_shapes=[pltpu.VMEM((third + 2 * PAD, lanes), jnp.float32)],
        compiler_params=params(),
        cost_estimate=cost(4e6, 3e6),
        name="pack_own",
    )(position.reshape(1), state, initial)
    first_low = hop(first, 1)
    first_high = hop(first, -1)
    own = lax.all_to_all(sent, "tm", split_axis=0, concat_axis=0, tiled=True)
    own = own.reshape(horizon, pairs, rows, lanes)

    sent_early = pl.pallas_call(
        pack_early,
        out_shape=shape_of(count, steps, taken, rows, lanes),
        in_specs=vmem(2),
        out_specs=pl.BlockSpec(memory_space=pltpu.VMEM),
        compiler_params=params(),
        cost_estimate=cost(4e6, 3e6),
        name="pack_early",
    )(lower, upper)

    up, down = pl.pallas_call(
        functools.partial(pack_late, skip),
        out_shape=(shape_of(horizon // 2, late, post_rows, lanes),) * 2,
        in_specs=vmem(1),
        out_specs=vmem(2),
        compiler_params=params(),
        cost_estimate=cost(2e6, 2e6),
        name="pack_late",
    )(own)
    late_low = hop(up, 1)
    late_high = hop(down, -1)

    early = lax.all_to_all(sent_early, "tm", split_axis=0, concat_axis=0, tiled=True)
    early = early.reshape(horizon, taken, rows, lanes)

    carried = lax.ppermute(state[steps - 1], "tm", [(i, i + 1) for i in range(count - 1)])
    carried = jnp.where(position == 0, initial, carried)
    residual = pl.pallas_call(
        residual_of,
        out_shape=shape_of(*state.shape),
        in_specs=vmem(4),
        out_specs=pl.BlockSpec(memory_space=pltpu.VMEM),
        compiler_params=params(),
        cost_estimate=cost(6e6, 3e6),
        name="residual",
    )(state, carried, lower[:, taken - 1], upper[:, 0])

    scratch_rows = rows + 2 * PAD
    layers = depth + pairs + 1
    any_space = pl.BlockSpec(memory_space=pl.ANY)
    moved = pl.pallas_call(
        functools.partial(solve, skip),
        out_shape=shape_of(horizon, pairs, size, lanes),
        in_specs=[pl.BlockSpec(memory_space=pltpu.SMEM)] + vmem(5) + [any_space] * 2,
        out_specs=pl.BlockSpec(memory_space=pltpu.VMEM),
        scratch_shapes=[
            pltpu.VMEM((horizon + 1, layers, scratch_rows, lanes), jnp.float32),
            pltpu.VMEM((horizon, layers, scratch_rows, lanes), jnp.float32),
            pltpu.VMEM((horizon, layers, scratch_rows, lanes), jnp.float32),
            pltpu.VMEM((horizon, layers, scratch_rows, lanes), jnp.float32),
            pltpu.SemaphoreType.DMA((2,)),
        ],
        compiler_params=params(),
        cost_estimate=cost(1e8, 8e6),
        name="solve",
    )(jnp.asarray(sweep_table(horizon)), late_low, late_high, first, first_low, first_high, own, early)

    moved = moved.reshape(count, steps, pairs, size, lanes)
    pieces = lax.all_to_all(moved, "tm", split_axis=0, concat_axis=0, tiled=True)
    updated = pl.pallas_call(
        finish,
        out_shape=shape_of(*state.shape),
        in_specs=vmem(2),
        out_specs=pl.BlockSpec(memory_space=pltpu.VMEM),
        compiler_params=params(),
        cost_estimate=cost(2e6, 3e6),
        name="finish",
    )(state, pieces)
    return (updated, residual)


def solution(mesh):
    in_specs = (P("tm", "space", None, None), P("space", None, None))
    out_specs = (P("tm", "space", None, None), P("tm", "space", None, None))
    return jax.shard_map(body, mesh=mesh, in_specs=in_specs, out_specs=out_specs, check_vma=False)
```

```python
import functools
import math

import jax
import jax.numpy as jnp
import numpy as np
from jax import lax
from jax.experimental import pallas as pl
from jax.experimental.pallas import tpu as pltpu
from jax.sharding import PartitionSpec as P


SWEEPS = 6
EARLY = 3

alpha_value = 0.1
time_step = 0.1
couple_first = 0.4
couple_cross = 0.05
reaction_shift = 0.1
relaxation = 0.9

CHUNK = 16
LANES = 128
PAD = 8
MIB = 1024 * 1024


def ring(axis, step):
    count = lax.axis_size(axis)
    return [(i, (i + step) % count) for i in range(count)]


def hop(block, step):
    return lax.ppermute(block, "space", ring("space", step))


def tile_of(low, high, mix):
    second, third = low.shape
    parts = []
    for part in range(third // LANES):
        here = slice(part * LANES, (part + 1) * LANES)
        mix[part, pl.ds(0, second, stride=2), :] = low[:, here]
        mix[part, pl.ds(1, second, stride=2), :] = high[:, here]
        parts.append(mix[part].T)
    return jnp.concatenate(parts, axis=0)


def windows(tile, count):
    third = tile.shape[0]
    size = third // count
    padded = jnp.concatenate([tile[third - PAD :], tile, tile[:PAD]], axis=0)
    return [padded[b * size : b * size + size + 2 * PAD] for b in range(count)]


def pack_inner(start, state, out, mix):
    count, steps, pairs, _, _ = out.shape
    width = state.shape[1]
    for pair in range(pairs):
        for step in range(steps):
            low, high = state[step, start + pair], state[step, width - 1 - start - pair]
            for b, window in enumerate(windows(tile_of(low, high, mix.at[step % 2]), count)):
                out[b, step, pair] = window


def pack_outer(position, state, initial, out, first, stage, mix):
    count, rows = out.shape[0], out.shape[3]
    width = state.shape[1]
    third = state.shape[3]
    size = third // count
    pack_inner(0, state, out, mix)
    for pair in range(first.shape[0]):
        tile = tile_of(initial[pair], initial[width - 1 - pair], mix.at[0])
        stage[:PAD] = tile[third - PAD :]
        stage[PAD : PAD + third] = tile
        stage[PAD + third :] = tile[:PAD]
        first[pair] = stage[pl.ds(pl.multiple_of(position[0] * size, 8), rows), :]


def pack_early(lower, upper, out, mix):
    count, steps, depth, _, _ = out.shape
    for step in range(steps):
        for j in range(depth):
            tile = tile_of(lower[step, j], upper[step, depth - 1 - j], mix.at[j % 2])
            for b, window in enumerate(windows(tile, count)):
                out[b, step, j] = window


def low_mask(tile):
    return lax.broadcasted_iota(jnp.int32, tile.shape, tile.ndim - 1) % 2 == 0


def swap(tile):
    lanes, axis = tile.shape[-1], tile.ndim - 1
    return jnp.where(low_mask(tile), pltpu.roll(tile, lanes - 1, axis), pltpu.roll(tile, 1, axis))


def pack_late(skip, pairs, start, own, up, down):
    half, late, rows, _ = up.shape
    width = 2 * pairs
    depth = SWEEPS

    def step(t, carry):
        for j in range(late):
            a = depth - j
            for out, layer in ((up, width - a), (down, a - 1)):
                pair, in_low = (layer, True) if layer < pairs else (width - 1 - layer, False)
                early = own[t, pair - start, skip : skip + rows]
                later = own[t + half, pair - start, skip : skip + rows]
                if in_low:
                    out[t, j] = jnp.where(low_mask(early), early, swap(later))
                else:
                    out[t, j] = jnp.where(low_mask(early), swap(early), later)
        return carry

    lax.fori_loop(0, half, step, 0)


def real_forward(values):
    count = len(values)
    if count == 1:
        return [(values[0], None)]
    if count == 2:
        return [(values[0] + values[1], None), (values[0] - values[1], None)]
    even = real_forward(values[0::2])
    odd = real_forward(values[1::2])
    half = count // 2
    result = [None] * (half + 1)
    for k in range(count // 4 + 1):
        even_real, even_imag = even[k]
        odd_real, odd_imag = odd[k]
        if k == 0:
            result[0] = (even_real + odd_real, None)
            result[half] = (even_real - odd_real, None)
        elif 4 * k == count:
            result[k] = (even_real, -odd_real)
        else:
            cos, sin = math.cos(2 * math.pi * k / count), math.sin(2 * math.pi * k / count)
            if odd_imag is None:
                turned_real, turned_imag = cos * odd_real, -sin * odd_real
            else:
                turned_real = cos * odd_real + sin * odd_imag
                turned_imag = cos * odd_imag - sin * odd_real
            if even_imag is None:
                result[k] = (even_real + turned_real, turned_imag)
                result[half - k] = (even_real - turned_real, turned_imag)
            else:
                result[k] = (even_real + turned_real, even_imag + turned_imag)
                result[half - k] = (even_real - turned_real, turned_imag - even_imag)
    return result


def real_inverse(modes):
    half = len(modes) - 1
    count = 2 * half
    if count == 2:
        return [modes[0][0] + modes[1][0], modes[0][0] - modes[1][0]]
    even, odd = [], []
    for k in range(count // 4 + 1):
        real, imag = modes[k]
        other_real, other_imag = modes[half - k]
        if k == 0:
            even.append((real + other_real, None))
            odd.append((real - other_real, None))
        elif 4 * k == count:
            even.append((2.0 * real, None))
            odd.append((-2.0 * imag, None))
        else:
            cos, sin = math.cos(2 * math.pi * k / count), math.sin(2 * math.pi * k / count)
            even.append((real + other_real, imag - other_imag))
            minus_real, minus_imag = real - other_real, imag + other_imag
            odd.append((cos * minus_real - sin * minus_imag, sin * minus_real + cos * minus_imag))
    result = [None] * count
    result[0::2] = real_inverse(even)
    result[1::2] = real_inverse(odd)
    return result


def mode_inverses(horizon):
    rho = alpha_value ** (1.0 / horizon)
    angles = 2.0 * math.pi * np.arange(horizon // 2 + 1) / horizon
    shift = (
        1.0 + reaction_shift + 2.0 * couple_first + 4.0 * couple_cross - rho * np.cos(angles)
    ) + 1j * rho * np.sin(angles)
    return 1.0 / shift


def sweep_table(horizon):
    inverse = relaxation * mode_inverses(horizon)
    rows = [(inverse[0].real, 0.0, 0.0, inverse[-1].real)]
    rows += [(v.real, -v.imag, v.imag, v.real) for v in inverse[1:-1]]
    return couple_cross * np.array(rows, np.float32)


def second_sum(tile):
    lanes, axis = tile.shape[-1], tile.ndim - 1
    return pltpu.roll(tile, 2, axis) + pltpu.roll(tile, lanes - 2, axis)


def solve(
    skip, table, up, down, first, first_low, first_high, outer, inner, early, out, state, base, ping, pong, sems
):
    horizon = inner.shape[0]
    pairs = first.shape[0]
    start = outer.shape[1]
    taken = early.shape[1]
    depth = SWEEPS
    late = depth - taken
    rows = inner.shape[2]
    post_rows = up.shape[2]
    block = rows - 2 * PAD
    last = depth + pairs - 1
    half = horizon // 2
    at = PAD
    copies = [
        pltpu.make_async_copy(
            outer, state.at[pl.ds(1, horizon), pl.ds(depth, start), pl.ds(at, rows)], sems.at[0]
        ),
        pltpu.make_async_copy(
            inner,
            state.at[pl.ds(1, horizon), pl.ds(depth + start, pairs - start), pl.ds(at, rows)],
            sems.at[2],
        ),
        pltpu.make_async_copy(
            early, state.at[pl.ds(1, horizon), pl.ds(late, taken), pl.ds(at, rows)], sems.at[1]
        ),
    ]
    for copy in copies:
        copy.start()

    for i in range(pairs):
        state[0, depth + i, at : at + rows] = first[i]
    for a in range(1, depth):
        if a <= pairs:
            low, high = first_low[a - 1], first_high[a - 1]
            tile = swap(jnp.where(low_mask(low), high, low))
        else:
            low, high = first_low[2 * pairs - a], first_high[2 * pairs - a]
            tile = jnp.where(low_mask(low), low, high)
        state[0, depth - a, at : at + rows] = tile

    def place(t, carry):
        for j in range(late):
            low, high = up[t, j], down[t, j]
            mask = low_mask(low)
            here = slice(at + skip, at + skip + post_rows)
            state[1 + t, j, here] = jnp.where(mask, low, swap(high))
            state[1 + half + t, j, here] = jnp.where(mask, swap(low), high)
        return carry

    lax.fori_loop(0, half, place, 0)
    for copy in copies:
        copy.wait()

    def mirror(t, carry):
        state[t, last + 1, at : at + rows] = swap(state[t, last, at : at + rows])
        return carry

    lax.fori_loop(0, horizon + 1, mirror, 0)

    def weigh(t, carry):
        centre = time_step - 1.0 - 2.0 * couple_first - 4.0 * couple_cross
        for x in range(1, last + 1):
            for r in range(at, at + rows, CHUNK):
                s = state[t + 1, x, r : r + CHUNK]
                along = state[t + 1, x - 1, r : r + CHUNK] + state[t + 1, x + 1, r : r + CHUNK]
                across = (
                    state[t + 1, x, r - 1 : r + CHUNK - 1]
                    + state[t + 1, x, r + 1 : r + CHUNK + 1]
                    + second_sum(s)
                )
                ping[t, x, r : r + CHUNK] = (
                    (state[t, x, r : r + CHUNK] + couple_first * along)
                    + (couple_cross * across + s * (centre - time_step * (s * s)))
                )
        return carry

    lax.fori_loop(0, horizon, weigh, 0)

    inverses = mode_inverses(horizon)
    weights = [alpha_value ** (n / horizon) for n in range(horizon)]
    tiles = rows // 8

    def transform(index, carry):
        x = 1 + index // tiles
        r = pl.ds(pl.multiple_of(at + (index % tiles) * 8, 8), 8)
        spectrum = real_forward([weights[n] * ping[n, x, r, :] for n in range(horizon)])
        for k, (real, imag) in enumerate(spectrum):
            c = relaxation * inverses[k]
            if k == 0:
                base[0, x, r, :] = float(c.real) * real
            elif k == half:
                base[half, x, r, :] = float(c.real) * real
            else:
                base[k, x, r, :] = float(c.real) * real - float(c.imag) * imag
                base[half + k, x, r, :] = float(c.imag) * real + float(c.real) * imag
        return carry

    lax.fori_loop(0, last * tiles, transform, 0)

    def mirror_base(k, carry):
        base[k, last + 1, at : at + rows] = swap(base[k, last, at : at + rows])
        return carry

    lax.fori_loop(0, horizon, mirror_base, 0)

    def sweep(number, source, target):
        reach = SWEEPS - 1 - number
        begin = at + PAD - 8 * (-(-reach // 8))
        chunks = (block + 2 * (at + PAD - begin)) // CHUNK

        def pair(k, carry):
            a, b, c, d = [table[k, i] for i in range(4)]
            for x in range(number + 1, last + 1):
                for chunk in range(chunks):
                    r = begin + chunk * CHUNK
                    near = []
                    for m in (k, half + k):
                        v = source[m, x, r : r + CHUNK]
                        along = source[m, x - 1, r : r + CHUNK] + source[m, x + 1, r : r + CHUNK]
                        across = (
                            source[m, x, r - 1 : r + CHUNK - 1]
                            + source[m, x, r + 1 : r + CHUNK + 1]
                            + second_sum(v)
                        )
                        near.append(
                            (
                                base[m, x, r : r + CHUNK] + (1.0 - relaxation) * v,
                                (couple_first / couple_cross) * along + across,
                            )
                        )
                    (rest_real, near_real), (rest_imag, near_imag) = near
                    real = rest_real + (a * near_real + b * near_imag)
                    imag = rest_imag + (c * near_real + d * near_imag)
                    target[k, x, r : r + CHUNK] = real
                    target[half + k, x, r : r + CHUNK] = imag
                    if x == last:
                        target[k, last + 1, r : r + CHUNK] = swap(real)
                        target[half + k, last + 1, r : r + CHUNK] = swap(imag)
            return carry

        lax.fori_loop(0, half, pair, 0)

    source = base
    for number in range(1, SWEEPS):
        target = ping if number % 2 else pong
        sweep(number, source, target)
        source = target

    kept = block // 8

    def restore(index, carry):
        i = index // kept
        r = pl.ds(pl.multiple_of(at + PAD + (index % kept) * 8, 8), 8)
        modes = [(source[0, depth + i, r, :], None)]
        modes += [
            (source[k, depth + i, r, :], source[half + k, depth + i, r, :]) for k in range(1, half)
        ]
        modes += [(source[half, depth + i, r, :], None)]
        place_at = pl.ds(pl.multiple_of((index % kept) * 8, 8), 8)
        for n, value in enumerate(real_inverse(modes)):
            out[n, i, place_at, :] = (1.0 / (horizon * weights[n])) * value
        return carry

    lax.fori_loop(0, pairs * kept, restore, 0)


def finish(state, pieces, updated, mix):
    count, steps, pairs, _, lanes = pieces.shape
    width = 2 * pairs
    second = lanes // 2
    for step in range(steps):
        for pair in range(pairs):
            tile = jnp.concatenate([pieces[b, step, pair] for b in range(count)], axis=0).T
            mirror = width - 1 - pair
            for part in range(tile.shape[1] // LANES):
                here = slice(part * LANES, (part + 1) * LANES)
                piece = mix.at[pair % 2, part]
                piece[...] = tile[:, here]
                low, high = piece[pl.ds(0, second, stride=2), :], piece[pl.ds(1, second, stride=2), :]
                updated[step, pair, :, here] = state[step, pair, :, here] + low
                updated[step, mirror, :, here] = state[step, mirror, :, here] + high


def residual_of(state, carried, low, high, out):
    steps, width = state.shape[:2]
    for step in range(steps):
        for layer in range(width):
            s = state[step, layer]
            below = low[step] if layer == 0 else state[step, layer - 1]
            above = high[step] if layer == width - 1 else state[step, layer + 1]
            before = carried[layer] if step == 0 else state[step - 1, layer]
            across = (
                pltpu.roll(s, 1, 0)
                + pltpu.roll(s, s.shape[0] - 1, 0)
                + pltpu.roll(s, 1, 1)
                + pltpu.roll(s, s.shape[1] - 1, 1)
            )
            centre = time_step - 1.0 - 2.0 * couple_first - 4.0 * couple_cross
            out[step, layer] = (
                (before + couple_first * (below + above))
                + (couple_cross * across + s * (centre - time_step * (s * s)))
            )


def vmem(count):
    return [pl.BlockSpec(memory_space=pltpu.VMEM)] * count


def shape_of(*dims):
    return jax.ShapeDtypeStruct(dims, jnp.float32)


def params(*arrays):
    held = sum(4 * math.prod(getattr(a, "shape", a)) for a in arrays)
    return pltpu.CompilerParams(vmem_limit_bytes=held + 2 * MIB)


def cost(flops, bytes_accessed):
    return pl.CostEstimate(flops=int(flops), bytes_accessed=int(bytes_accessed), transcendentals=0)


def exchange(block):
    return lax.all_to_all(block, "tm", split_axis=0, concat_axis=0, tiled=True)


def iteration(state, initial):
    steps, width, second, third = state.shape
    count = lax.axis_size("tm")
    horizon = steps * count
    position = lax.axis_index("tm")
    depth, taken = SWEEPS, EARLY
    late = depth - taken
    pairs = width // 2
    start = min(taken, width - depth)
    size = third // count
    rows = size + 2 * PAD
    lanes = 2 * second
    skip = 4
    post_rows = rows - 2 * skip
    mixer = pltpu.VMEM((2, third // LANES, lanes, LANES), jnp.float32)

    lower = hop(state[:, width - taken :], 1)
    upper = hop(state[:, :taken], -1)

    sent_inner = pl.pallas_call(
        functools.partial(pack_inner, start),
        out_shape=shape_of(count, steps, pairs - start, rows, lanes),
        in_specs=vmem(1),
        out_specs=pl.BlockSpec(memory_space=pltpu.VMEM),
        scratch_shapes=[mixer],
        compiler_params=params(state, state, state),
        cost_estimate=cost(4e6, 3e6),
        name="pack_inner",
    )(state)
    inner = exchange(sent_inner).reshape(horizon, pairs - start, rows, lanes)

    sent_outer, first = pl.pallas_call(
        pack_outer,
        out_shape=(shape_of(count, steps, start, rows, lanes), shape_of(pairs, rows, lanes)),
        in_specs=[pl.BlockSpec(memory_space=pltpu.SMEM)] + vmem(2),
        out_specs=vmem(2),
        scratch_shapes=[pltpu.VMEM((third + 2 * PAD, lanes), jnp.float32), mixer],
        compiler_params=params(state, state, initial, state),
        cost_estimate=cost(4e6, 3e6),
        name="pack_outer",
    )(position.reshape(1), state, initial)
    outer = exchange(sent_outer).reshape(horizon, start, rows, lanes)
    first_low = hop(first, 1)
    first_high = hop(first, -1)

    up, down = pl.pallas_call(
        functools.partial(pack_late, skip, pairs, start),
        out_shape=(shape_of(horizon // 2, late, post_rows, lanes),) * 2,
        in_specs=vmem(1),
        out_specs=vmem(2),
        compiler_params=params(inner, inner),
        cost_estimate=cost(2e6, 2e6),
        name="pack_late",
    )(inner)
    late_low = hop(up, 1)
    late_high = hop(down, -1)

    sent_early = pl.pallas_call(
        pack_early,
        out_shape=shape_of(count, steps, taken, rows, lanes),
        in_specs=vmem(2),
        out_specs=pl.BlockSpec(memory_space=pltpu.VMEM),
        scratch_shapes=[mixer],
        compiler_params=params(lower, upper, sent_inner, sent_outer),
        cost_estimate=cost(4e6, 3e6),
        name="pack_early",
    )(lower, upper)
    early = exchange(sent_early).reshape(horizon, taken, rows, lanes)

    carried = lax.ppermute(state[steps - 1], "tm", [(i, i + 1) for i in range(count - 1)])
    carried = jnp.where(position == 0, initial, carried)
    residual = pl.pallas_call(
        residual_of,
        out_shape=shape_of(*state.shape),
        in_specs=vmem(4),
        out_specs=pl.BlockSpec(memory_space=pltpu.VMEM),
        compiler_params=params(state, state, carried, lower),
        cost_estimate=cost(6e6, 3e6),
        name="residual",
    )(state, carried, lower[:, taken - 1], upper[:, 0])

    scratch_rows = rows + 2 * PAD
    layers = depth + pairs + 1
    any_space = pl.BlockSpec(memory_space=pl.ANY)
    moved = pl.pallas_call(
        functools.partial(solve, skip),
        out_shape=shape_of(horizon, pairs, size, lanes),
        in_specs=[pl.BlockSpec(memory_space=pltpu.SMEM)] + vmem(5) + [any_space] * 3,
        out_specs=pl.BlockSpec(memory_space=pltpu.VMEM),
        scratch_shapes=[
            pltpu.VMEM((horizon + 1, layers, scratch_rows, lanes), jnp.float32),
            pltpu.VMEM((horizon, layers, scratch_rows, lanes), jnp.float32),
            pltpu.VMEM((horizon, layers, scratch_rows, lanes), jnp.float32),
            pltpu.VMEM((horizon, layers, scratch_rows, lanes), jnp.float32),
            pltpu.SemaphoreType.DMA((3,)),
        ],
        compiler_params=params((4 * MIB,), *[(horizon + 1, layers, scratch_rows, lanes)] * 4),
        cost_estimate=cost(1e8, 8e6),
        name="solve",
    )(
        jnp.asarray(sweep_table(horizon)),
        late_low,
        late_high,
        first,
        first_low,
        first_high,
        outer,
        inner,
        early,
    )

    moved = moved.reshape(count, steps, pairs, size, lanes)
    pieces = exchange(moved)
    updated = pl.pallas_call(
        finish,
        out_shape=shape_of(*state.shape),
        in_specs=vmem(2),
        out_specs=pl.BlockSpec(memory_space=pltpu.VMEM),
        scratch_shapes=[mixer],
        compiler_params=params(state, state, state),
        cost_estimate=cost(2e6, 3e6),
        name="finish",
    )(state, pieces)
    return (updated, residual)


def solution(mesh):
    in_specs = (P("tm", "space", None, None), P("space", None, None))
    out_specs = (P("tm", "space", None, None), P("tm", "space", None, None))
    return jax.shard_map(iteration, mesh=mesh, in_specs=in_specs, out_specs=out_specs, check_vma=False)
```

```python
import functools
import math

import jax
import jax.numpy as jnp
import numpy as np
from jax import lax
from jax.experimental import pallas as pl
from jax.experimental.pallas import tpu as pltpu
from jax.sharding import PartitionSpec as P


SWEEPS = 6
EARLY = 3

alpha_value = 0.1
time_step = 0.1
couple_first = 0.4
couple_cross = 0.05
reaction_shift = 0.1
relaxation = 0.9

CHUNK = 8
LANES = 128
PAD = 8
EDGE = 12
MIB = 1024 * 1024


def reach(depth):
    return SWEEPS - max(depth, 0)


def ring(axis, step):
    count = lax.axis_size(axis)
    return [(i, (i + step) % count) for i in range(count)]


def hop(block, step):
    return lax.ppermute(block, "space", ring("space", step))


def low_mask(tile):
    return lax.broadcasted_iota(jnp.int32, tile.shape, tile.ndim - 1) % 2 == 0


def first_mask(tile):
    return lax.broadcasted_iota(jnp.int32, tile.shape, tile.ndim - 1) // 2 % 2 == 0


def turn(tile, step):
    return pltpu.roll(tile, step % tile.shape[-1], tile.ndim - 1)


def merge(low, high, low_at=0, high_at=1):
    low = turn(low, -1) if low_at else low
    high = high if high_at else turn(high, 1)
    return jnp.where(low_mask(low), low, high)


def swap(tile):
    return jnp.where(low_mask(tile), turn(tile, -1), turn(tile, 1))


def stage_tile(mix, stage):
    third = mix.shape[0] * LANES
    for part in range(mix.shape[0]):
        stage[PAD + part * LANES : PAD + (part + 1) * LANES] = mix[part].T
    stage[:PAD] = stage[third : third + PAD]
    stage[third + PAD :] = stage[PAD : 2 * PAD]


def layer_half(layer, width):
    return (layer, True) if 2 * layer < width else (width - 1 - layer, False)


def copy_in(sems, pairs):
    copies = [pltpu.make_async_copy(a, b, sems.at[i]) for i, (a, b) in enumerate(pairs)]
    for copy in copies:
        copy.start()
    return copies


def pack_own(
    position, state_hbm, initial_hbm, out_hbm, first_hbm, up, down, state, initial, out, first, stage, mix, sems, out_sems
):
    count, steps = out.shape[:2]
    width, second, third = state.shape[1:]
    size = third // count
    pairs = width // 2
    rows = size + 2 * SWEEPS
    parts = third // LANES
    loads = []
    for pair in range(pairs):
        for i, layer in enumerate((pair, width - 1 - pair)):
            loads += copy_in(
                sems.at[pl.ds(4 * pair + 2 * i, 2)],
                [(state_hbm.at[:, layer], state.at[:, layer]), (initial_hbm.at[layer], initial.at[layer])],
            )
    stores = []
    for pair in range(pairs):
        for load in loads[4 * pair : 4 * pair + 4]:
            load.wait()
        for step in range(steps + 1):
            slot = step % 2
            for part in range(parts):
                here = slice(part * LANES, (part + 1) * LANES)
                for half, layer in enumerate((pair, width - 1 - pair)):
                    source = state[step, layer, :, here] if step < steps else initial[layer, :, here]
                    mix[slot, part, pl.ds(half, second, stride=2), :] = source
            stage_tile(mix.at[slot], stage.at[slot])
            if step < steps:
                for b in range(count):
                    begin = PAD - SWEEPS + b * size
                    out[b, step, pair * rows : (pair + 1) * rows] = stage[slot, begin : begin + rows]
            else:
                begin = pl.multiple_of(position[0] * size, 8)
                first[pair] = stage[slot, pl.ds(begin, size + 2 * PAD), :]
        if pair % 2:
            here = pl.ds((pair - 1) * rows, 2 * rows)
            stores += copy_in(
                out_sems.at[pl.ds(pair // 2, 1)], [(out.at[:, :, here], out_hbm.at[:, :, here])]
            )
    stores += copy_in(out_sems.at[pl.ds(pairs // 2, 1)], [(first, first_hbm)])
    at = 0
    for step in range(steps):
        for j in range(EARLY):
            for part in range(parts):
                here = slice(part * LANES, (part + 1) * LANES)
                up[at : at + second] = state[step, width - EARLY + j, :, here]
                down[at : at + second] = state[step, j, :, here]
                at += second
    short = size + 2 * (SWEEPS - 2)
    begin = PAD - SWEEPS + 2
    for slot in range(SWEEPS // 2):
        for out_ref, layers in (
            (up, [width - a for a in (2 * slot + 1, 2 * slot + 2)]),
            (down, [a - 1 for a in (2 * slot + 1, 2 * slot + 2)]),
        ):
            (one, one_low), (two, two_low) = [layer_half(layer, width) for layer in layers]
            out_ref[at : at + short] = merge(
                first[one, begin : begin + short],
                first[two, begin : begin + short],
                0 if one_low else 1,
                0 if two_low else 1,
            )
        at += short
    for store in stores:
        store.wait()


def early_rows(size):
    return [size + 2 * reach(EARLY - j) for j in range(EARLY)]


def late_rows(size):
    return [size + 2 * reach(SWEEPS - j) for j in range(SWEEPS - EARLY)]


def offsets(sizes):
    return [sum(sizes[:i]) for i in range(len(sizes))]


def pack_early(after, lower_hbm, upper_hbm, out_hbm, lower, upper, out, stage, mix, sems):
    count, steps = out.shape[:2]
    used = lower.shape[0] // steps
    loads = []
    for step in range(steps):
        here = pl.ds(step * used, used)
        loads += copy_in(
            sems.at[pl.ds(2 * step, 2)],
            [(lower_hbm.at[here], lower.at[here]), (upper_hbm.at[here], upper.at[here])],
        )
    parts = mix.shape[1]
    second = mix.shape[2] // 2
    size = parts * LANES // count
    sizes = early_rows(size)
    stores = []
    for step in range(steps):
        for load in loads[2 * step : 2 * step + 2]:
            load.wait()
        for j, (rows, at) in enumerate(zip(sizes, offsets(sizes))):
            slot = j % 2
            for part in range(parts):
                low = ((step * EARLY + j) * parts + part) * second
                high = ((step * EARLY + EARLY - 1 - j) * parts + part) * second
                mix[slot, part, pl.ds(0, second, stride=2), :] = lower[low : low + second]
                mix[slot, part, pl.ds(1, second, stride=2), :] = upper[high : high + second]
            stage_tile(mix.at[slot], stage.at[slot])
            for b in range(count):
                begin = PAD - (rows - size) // 2 + b * size
                out[b, step, at : at + rows] = stage[slot, begin : begin + rows]
        stores += copy_in(
            sems.at[pl.ds(2 * steps + step, 1)], [(out.at[:, step], out_hbm.at[:, step])]
        )
    for store in stores:
        store.wait()


def pack_late(pairs, size, own, up, down):
    horizon = own.shape[0]
    half = horizon // 2
    width = 2 * pairs
    stride = size + 2 * SWEEPS
    at = 0
    for j, rows in enumerate(late_rows(size)):
        a = SWEEPS - j
        for t in range(half):
            for out, layer in ((up, width - a), (down, a - 1)):
                pair, low = layer_half(layer, width)
                begin = pair * stride + (stride - rows) // 2
                before = own[t, begin : begin + rows]
                after = own[t + half, begin : begin + rows]
                here = 0 if low else 1
                out[at : at + rows] = merge(before, after, here, here)
            at += rows


def real_forward(values):
    count = len(values)
    if count == 1:
        return [(values[0], None)]
    if count == 2:
        return [(values[0] + values[1], None), (values[0] - values[1], None)]
    even = real_forward(values[0::2])
    odd = real_forward(values[1::2])
    half = count // 2
    result = [None] * (half + 1)
    for k in range(count // 4 + 1):
        even_real, even_imag = even[k]
        odd_real, odd_imag = odd[k]
        if k == 0:
            result[0] = (even_real + odd_real, None)
            result[half] = (even_real - odd_real, None)
        elif 4 * k == count:
            result[k] = (even_real, -odd_real)
        else:
            cos, sin = math.cos(2 * math.pi * k / count), math.sin(2 * math.pi * k / count)
            if odd_imag is None:
                turned_real, turned_imag = cos * odd_real, -sin * odd_real
            else:
                turned_real = cos * odd_real + sin * odd_imag
                turned_imag = cos * odd_imag - sin * odd_real
            if even_imag is None:
                result[k] = (even_real + turned_real, turned_imag)
                result[half - k] = (even_real - turned_real, turned_imag)
            else:
                result[k] = (even_real + turned_real, even_imag + turned_imag)
                result[half - k] = (even_real - turned_real, turned_imag - even_imag)
    return result


def real_inverse(modes):
    half = len(modes) - 1
    count = 2 * half
    if count == 2:
        return [modes[0][0] + modes[1][0], modes[0][0] - modes[1][0]]
    even, odd = [], []
    for k in range(count // 4 + 1):
        real, imag = modes[k]
        other_real, other_imag = modes[half - k]
        if k == 0:
            even.append((real + other_real, None))
            odd.append((real - other_real, None))
        elif 4 * k == count:
            even.append((2.0 * real, None))
            odd.append((-2.0 * imag, None))
        else:
            cos, sin = math.cos(2 * math.pi * k / count), math.sin(2 * math.pi * k / count)
            even.append((real + other_real, imag - other_imag))
            minus_real, minus_imag = real - other_real, imag + other_imag
            odd.append((cos * minus_real - sin * minus_imag, sin * minus_real + cos * minus_imag))
    result = [None] * count
    result[0::2] = real_inverse(even)
    result[1::2] = real_inverse(odd)
    return result


def mode_inverses(horizon):
    rho = alpha_value ** (1.0 / horizon)
    angles = 2.0 * math.pi * np.arange(horizon // 2 + 1) / horizon
    shift = (
        1.0 + reaction_shift + 2.0 * couple_first + 4.0 * couple_cross - rho * np.cos(angles)
    ) + 1j * rho * np.sin(angles)
    return 1.0 / shift


def sweep_table(horizon, lanes):
    inverse = relaxation * mode_inverses(horizon)
    rows = [(inverse[0].real, 0.0, 0.0, inverse[-1].real)]
    rows += [(v.real, -v.imag, v.imag, v.real) for v in inverse[1:-1]]
    table = couple_cross * np.array(rows)
    quarter = horizon // 4
    mode = np.arange(quarter)[:, None] + quarter * (np.arange(lanes) // 2 % 2)[None, :]
    spread = np.moveaxis(table[mode], -1, 1)[:, :, None, :]
    return np.broadcast_to(spread, (quarter, 4, 8, lanes)).astype(np.float32)


class Plan:
    def __init__(self, pairs):
        self.last = SWEEPS + pairs - 1
        self.begins = [SWEEPS, SWEEPS - EARLY, 0]

    def fresh(self, phase):
        end = self.last if phase == 0 else self.begins[phase - 1]
        return range(self.begins[phase] + 1, end + 1)

    def rows(self, phase, level):
        fresh = self.fresh(phase)
        return range(fresh.start + level, min(fresh.stop - 1 + level, self.last) + 1)

    def arrays(self, phase):
        return [(phase, level) for level in range(SWEEPS) if self.rows(phase, level)]

    def find(self, phase, level, row):
        for p in range(phase, -1, -1):
            if row in self.rows(p, level):
                return (p, level), row - self.rows(p, level).start
        raise ValueError((phase, level, row))

    def needed(self, phase):
        keys = set()
        for level in range(1, SWEEPS):
            for row in self.rows(phase, level):
                keys.add(self.find(phase, 0, row)[0])
                for x in (row - 1, row, min(row + 1, self.last)):
                    keys.add(self.find(phase, level - 1, x)[0])
        if phase == 2:
            for row in range(SWEEPS, self.last + 1):
                keys.add(self.find(phase, SWEEPS - 1, row)[0])
        return sorted(k for k in keys if k[0] < phase)

    def shape(self, key, horizon, size, lanes):
        rows = size + 2 * EDGE
        return (horizon, len(self.rows(*key)), rows, lanes)


def loop(count, copies, step):
    while count % copies:
        copies -= 1

    def several(index, carry):
        for i in range(copies):
            step(index * copies + i, 0)
        return carry

    lax.fori_loop(0, count // copies, several, 0)


def second_sum(tile):
    return turn(tile, 2) + turn(tile, -2)


def solve(phase, plan, pairs, size, names, far, *refs):
    named = dict(zip(names, refs))
    outs = refs[len(names) :]
    state, weighted, sems = refs[-3:]
    near = refs[-3 - len(far) : -3]
    halo = (SWEEPS // 2) * (size + 2 * (SWEEPS - 2))
    sources = {}
    for name in far:
        sources[name] = named[name]
        if name in ("first_low", "first_high"):
            sources[name] = named[name].at[pl.ds(named[name].shape[0] - halo, halo)]
    loads = dict(zip(far, copy_in(sems, [(sources[n], r) for n, r in zip(far, near)])))
    named |= dict(zip(far, near))
    horizon = weighted.shape[0]
    half, quarter = horizon // 2, horizon // 4
    last = plan.last
    window = size + 2 * EDGE
    at = PAD
    fresh = plan.fresh(phase)
    held = range(fresh.start - 1, fresh.stop + 1)
    keys = plan.arrays(phase)
    count = len(keys)
    results = outs[:1] if phase == 2 else outs[:count]
    inner_refs = refs[len(names) + len(results) :][:count] if phase != 1 else results
    final = refs[len(names) + 1 + count] if phase == 2 else None
    arrays = dict(zip(keys, inner_refs))
    for key in plan.needed(phase):
        arrays[key] = named[key]

    own, early, first = named["own"], named.get("early"), named["first"]
    early_sizes, late_sizes = early_rows(size), late_rows(size)
    early_at, late_at = offsets(early_sizes), offsets([half * rows for rows in late_sizes])
    late_count = SWEEPS - EARLY
    own_rows = size + 2 * SWEEPS

    def fill(t, carry):
        for x in held:
            if x > last:
                continue
            if x >= SWEEPS:
                begin = at + EDGE - SWEEPS
                state[1 + t, x - held.start, begin : begin + own_rows] = own[
                    t, (x - SWEEPS) * own_rows : (x - SWEEPS + 1) * own_rows
                ]
            elif x >= late_count:
                j = x - late_count
                begin = at + EDGE - (early_sizes[j] - size) // 2
                state[1 + t, x - held.start, begin : begin + early_sizes[j]] = early[
                    t, early_at[j] : early_at[j] + early_sizes[j]
                ]
        return carry

    loop(horizon, 4, fill)
    for x in held:
        if x < late_count:
            rows, where = late_sizes[x], late_at[x]
            begin = at + EDGE - (rows - size) // 2
            for t in range(half):
                low = named["late_low"][where + t * rows : where + (t + 1) * rows]
                high = named["late_high"][where + t * rows : where + (t + 1) * rows]
                state[1 + t, x - held.start, begin : begin + rows] = merge(low, high, 0, 0)
                state[1 + half + t, x - held.start, begin : begin + rows] = merge(low, high, 1, 1)
    for name in ("first", "first_low", "first_high"):
        if name in loads:
            loads.pop(name).wait()
    for x in fresh:
        if x >= SWEEPS:
            begin = at + EDGE - PAD
            state[0, x - held.start, begin : begin + size + 2 * PAD] = first[x - SWEEPS]
        else:
            a = SWEEPS - x
            rows = size + 2 * (SWEEPS - 2)
            total = named["first_low"].shape[0]
            where = total - (SWEEPS // 2 - (a - 1) // 2) * rows
            low, high = named["first_low"][where : where + rows], named["first_high"][where : where + rows]
            slot = (a - 1) % 2
            tile = merge(low, high, slot, slot)
            begin = at + EDGE - SWEEPS + 2
            state[0, x - held.start, begin : begin + rows] = tile

    def weigh(t, carry):
        centre = time_step - 1.0 - 2.0 * couple_first - 4.0 * couple_cross
        for i in range(len(fresh)):
            for r in range(at, at + window, CHUNK):
                s = state[t + 1, i + 1, r : r + CHUNK]
                outer = state[t + 1, i, r : r + CHUNK]
                along = outer + (swap(s) if fresh[i] == last else state[t + 1, i + 2, r : r + CHUNK])
                across = (
                    state[t + 1, i + 1, r - 1 : r + CHUNK - 1]
                    + state[t + 1, i + 1, r + 1 : r + CHUNK + 1]
                    + second_sum(s)
                )
                weighted[t, i, r - at : r - at + CHUNK] = (
                    (state[t, i + 1, r : r + CHUNK] + couple_first * along)
                    + (couple_cross * across + s * (centre - time_step * (s * s)))
                )
        return carry

    loop(horizon, 4, weigh)

    inverses = mode_inverses(horizon)
    weights = [alpha_value ** (n / horizon) for n in range(horizon)]
    tiles = window // 8
    base = arrays[(phase, 0)]

    def transform(index, carry):
        i = index // tiles
        r = pl.ds(pl.multiple_of((index % tiles) * 8, 8), 8)
        spectrum = real_forward([weights[n] * weighted[n, i, r, :] for n in range(horizon)])
        reals, imags = [None] * half, [None] * half
        for k, (real, imag) in enumerate(spectrum):
            c = relaxation * inverses[k]
            if k == 0:
                reals[0] = float(c.real) * real
            elif k == half:
                imags[0] = float(c.real) * real
            else:
                reals[k] = float(c.real) * real - float(c.imag) * imag
                imags[k] = float(c.imag) * real + float(c.real) * imag
        for part, values in enumerate((reals, imags)):
            for k in range(quarter):
                one, two = values[k], values[k + quarter]
                mask = first_mask(one)
                base[part * half + 2 * k, i, r, :] = jnp.where(mask, one, turn(two, 2))
                base[part * half + 2 * k + 1, i, r, :] = jnp.where(mask, turn(one, -2), two)
        return carry

    loop(len(fresh) * tiles, 3, transform)

    table = named["table"]
    for load in loads.values():
        load.wait()

    def sweep(level):
        rows = plan.rows(phase, level)
        span = size + PAD
        begin = EDGE - PAD // 2
        target = arrays[(phase, level)]

        def read(level_, part, k, parity, x, r):
            key, i = plan.find(phase, level_, x)
            return arrays[key][part * half + 2 * k + parity, i, r : r + CHUNK]

        def mode(k, carry):
            a, b, c, d = [table[k, i] for i in range(4)]
            for x in rows:
                for r in range(begin, begin + span, CHUNK):
                    for parity in (0, 1):
                        near = []
                        for part in (0, 1):
                            v = read(level - 1, part, k, parity, x, r)
                            other = read(level - 1, part, k, 1 - parity, x, r)
                            inner = (
                                swap(v)
                                if x == last
                                else read(level - 1, part, k, parity, x + 1, r)
                            )
                            along = read(level - 1, part, k, parity, x - 1, r) + inner
                            across = (
                                read(level - 1, part, k, parity, x, r - 1)
                                + read(level - 1, part, k, parity, x, r + 1)
                            ) + (other + turn(other, 4 if parity == 0 else -4))
                            near.append(
                                (
                                    read(0, part, k, parity, x, r) + (1.0 - relaxation) * v,
                                    (couple_first / couple_cross) * along + across,
                                )
                            )
                        (rest_real, near_real), (rest_imag, near_imag) = near
                        values = (
                            rest_real + (a * near_real + b * near_imag),
                            rest_imag + (c * near_real + d * near_imag),
                        )
                        here = slice(r, r + CHUNK)
                        for part, value in enumerate(values):
                            m = part * half + 2 * k + parity
                            target[m, x - rows.start, here] = value
            return carry

        loop(quarter, 2, mode)

    for key in keys:
        if key[1]:
            sweep(key[1])
    if phase == 0:
        for store in copy_in(sems, [(arrays[key], ref) for key, ref in zip(keys, results)]):
            store.wait()
    if phase < 2:
        return

    kept = size // 8
    done = [plan.find(phase, SWEEPS - 1, SWEEPS + i) for i in range(pairs)]
    stores = []
    for i, (key, row) in enumerate(done):

        for index in range(kept):
            source = arrays[key]
            r = slice(EDGE + index * 8, EDGE + index * 8 + 8)
            parts = []
            for part in (0, 1):
                values = [None] * half
                for k in range(quarter):
                    even = source[part * half + 2 * k, row, r, :]
                    odd = source[part * half + 2 * k + 1, row, r, :]
                    mask = first_mask(even)
                    values[k] = jnp.where(mask, even, turn(odd, 2))
                    values[k + quarter] = jnp.where(mask, turn(even, -2), odd)
                parts.append(values)
            reals, imags = parts
            modes = [(reals[0], None)] + list(zip(reals[1:], imags[1:])) + [(imags[0], None)]
            for n, value in enumerate(real_inverse(modes)):
                final[n, i, index * 8 : index * 8 + 8] = (1.0 / (horizon * weights[n])) * value
        stores += copy_in(sems.at[pl.ds(i, 1)], [(final.at[:, i], results[0].at[:, i])])
    for store in stores:
        store.wait()


def finish(state, pieces, updated, mix):
    count, steps, pairs, size, lanes = pieces.shape
    width = 2 * pairs
    second = lanes // 2
    per = LANES // size
    for step in range(steps):
        for pair in range(pairs):
            mirror = width - 1 - pair
            for part in range(count // per):
                here = slice(part * LANES, (part + 1) * LANES)
                piece = mix.at[pair % 2, part]
                piece[...] = jnp.concatenate(
                    [pieces[part * per + b, step, pair] for b in range(per)], axis=0
                ).T
                low, high = piece[pl.ds(0, second, stride=2), :], piece[pl.ds(1, second, stride=2), :]
                updated[step, pair, :, here] = state[step, pair, :, here] + low
                updated[step, mirror, :, here] = state[step, mirror, :, here] + high


def residual_of(state, carried, lower_hbm, upper_hbm, out, lower, upper, sems):
    steps, width, second, third = state.shape
    parts = third // LANES
    used = pl.ds(0, lower.shape[0])
    loads = copy_in(sems, [(lower_hbm.at[used], lower), (upper_hbm.at[used], upper)])
    for load in loads:
        load.wait()

    def outside(ref, step, j):
        at = (step * EARLY + j) * parts * second
        return jnp.concatenate(
            [ref[at + part * second : at + (part + 1) * second] for part in range(parts)], axis=1
        )

    for step in range(steps):
        for layer in range(width):
            s = state[step, layer]
            below = outside(lower, step, EARLY - 1) if layer == 0 else state[step, layer - 1]
            above = outside(upper, step, 0) if layer == width - 1 else state[step, layer + 1]
            before = carried[layer] if step == 0 else state[step - 1, layer]
            across = (
                pltpu.roll(s, 1, 0)
                + pltpu.roll(s, s.shape[0] - 1, 0)
                + pltpu.roll(s, 1, 1)
                + pltpu.roll(s, s.shape[1] - 1, 1)
            )
            centre = time_step - 1.0 - 2.0 * couple_first - 4.0 * couple_cross
            out[step, layer] = (
                (before + couple_first * (below + above))
                + (couple_cross * across + s * (centre - time_step * (s * s)))
            )


def shape_of(*dims):
    return jax.ShapeDtypeStruct(dims, jnp.float32)


def padded_bytes(shape):
    *major, rows, lanes = (1, 1, *shape)
    return 4 * math.prod(major) * (-(-rows // 8) * 8) * (-(-lanes // 128) * 128)


def call(kernel, outs, args, scratch=(), flops=2e6, scalars=0, far=(), far_outs=()):
    spaces = [
        pltpu.SMEM if i < scalars else pltpu.HBM if i in far else pltpu.VMEM for i in range(len(args))
    ]
    out_spaces = [pltpu.HBM if i in far_outs else pltpu.VMEM for i in range(len(outs))]
    held = [a.shape for i, a in enumerate(args) if i not in far]
    held += [o.shape for i, o in enumerate(outs) if i not in far_outs]
    held += [r.shape for r in scratch if len(r.shape) > 1]
    moved = sum(padded_bytes(a.shape) for a in (*args, *outs))
    args = [
        pltpu.with_memory_space_constraint(a, pltpu.HBM) if i in far else a for i, a in enumerate(args)
    ]
    outs = [pltpu.HBM(o.shape, o.dtype) if i in far_outs else o for i, o in enumerate(outs)]
    return pl.pallas_call(
        kernel,
        out_shape=tuple(outs),
        in_specs=[pl.BlockSpec(memory_space=space) for space in spaces],
        out_specs=tuple(pl.BlockSpec(memory_space=space) for space in out_spaces),
        scratch_shapes=list(scratch),
        compiler_params=pltpu.CompilerParams(
            vmem_limit_bytes=sum(padded_bytes(s) for s in held) + 2 * MIB
        ),
        cost_estimate=pl.CostEstimate(
            flops=int(flops), bytes_accessed=int(moved), transcendentals=0
        ),
    )(*args)


def vmem(*shape):
    return pltpu.VMEM(shape, jnp.float32)


def semaphores(count):
    return pltpu.SemaphoreType.DMA((count,))


def exchange(block):
    return lax.all_to_all(block, "tm", split_axis=0, concat_axis=0, tiled=True)


def iteration(state, initial):
    steps, width, second, third = state.shape
    count = lax.axis_size("tm")
    horizon = steps * count
    half = horizon // 2
    position = lax.axis_index("tm")
    pairs = width // 2
    size = third // count
    lanes = 2 * second
    stage = vmem(2, third + 2 * PAD, lanes)
    mixer = vmem(2, third // LANES, lanes, LANES)

    raw_rows = EARLY * steps * second * (third // LANES)
    sent_rows = raw_rows + (SWEEPS // 2) * (size + 2 * SWEEPS - 4)
    own_shape = (count, steps, pairs * (size + 2 * SWEEPS), lanes)
    first_shape = (pairs, size + 2 * PAD, lanes)
    sent, first, up, down = call(
        pack_own,
        [
            shape_of(*own_shape),
            shape_of(*first_shape),
            shape_of(sent_rows, LANES),
            shape_of(sent_rows, LANES),
        ],
        [position.reshape(1), state, initial],
        [
            vmem(*state.shape),
            vmem(*initial.shape),
            vmem(*own_shape),
            vmem(*first_shape),
            stage,
            mixer,
            semaphores(4 * pairs),
            semaphores(pairs // 2 + 1),
        ],
        scalars=1,
        far=(1, 2),
        far_outs=(0, 1),
    )
    own = exchange(sent).reshape(horizon, -1, lanes)

    lower = hop(up, 1)
    upper = hop(down, -1)

    late_shape = shape_of(half * sum(late_rows(size)), lanes)
    late_up, late_down = call(functools.partial(pack_late, pairs, size), [late_shape] * 2, [own])
    late_low = hop(late_up, 1)
    late_high = hop(late_down, -1)

    early_shape = (count, steps, sum(early_rows(size)), lanes)
    (sent_early,) = call(
        pack_early,
        [shape_of(*early_shape)],
        [late_up, lower, upper],
        [
            vmem(raw_rows, LANES),
            vmem(raw_rows, LANES),
            vmem(*early_shape),
            stage,
            mixer,
            semaphores(3 * steps),
        ],
        far=(0, 1, 2),
        far_outs=(0,),
    )
    early = exchange(sent_early).reshape(horizon, -1, lanes)

    carried = lax.ppermute(state[steps - 1], "tm", [(i, i + 1) for i in range(count - 1)])
    carried = jnp.where(position == 0, initial, carried)
    (residual,) = call(
        residual_of,
        [shape_of(*state.shape)],
        [state, carried, lower, upper],
        [vmem(raw_rows, LANES), vmem(raw_rows, LANES), semaphores(2)],
        flops=6e6,
        far=(2, 3),
    )

    plan = Plan(pairs)
    table = jnp.asarray(sweep_table(horizon, lanes))
    arrays = {}
    for phase in range(3):
        inputs = {"table": table, "own": own, "first": first}
        if phase:
            inputs |= {"early": early, "first_low": lower, "first_high": upper}
        if phase == 2:
            inputs |= {"late_low": late_low, "late_high": late_high}
        inputs |= {key: arrays[key] for key in plan.needed(phase)}
        keys = plan.arrays(phase)
        outs = [shape_of(*plan.shape(key, horizon, size, lanes)) for key in keys]
        fresh = len(plan.fresh(phase))
        halo = vmem((SWEEPS // 2) * (size + 2 * (SWEEPS - 2)), lanes)
        far = [n for n in inputs if n in ("first", "first_low", "first_high") or n[0] == 0]
        near = [halo if n[:6] == "first_" else vmem(*inputs[n].shape) for n in far]
        scratch = near + [
            vmem(horizon + 1, fresh + 2, size + 2 * EDGE + 2 * PAD, lanes),
            vmem(horizon, fresh, size + 2 * EDGE, lanes),
            semaphores(max(len(far), len(keys), pairs)),
        ]
        inner = [vmem(*o.shape) for o in outs]
        if phase == 0:
            scratch = inner + scratch
        if phase == 2:
            scratch = inner + [vmem(horizon, pairs, size, lanes)] + scratch
            outs = [shape_of(horizon, pairs, size, lanes)]
        results = call(
            functools.partial(solve, phase, plan, pairs, size, list(inputs), far),
            outs,
            list(inputs.values()),
            scratch,
            flops=3e7,
            far=[i for i, n in enumerate(inputs) if n in far],
            far_outs=() if phase == 1 else range(len(outs)),
        )
        arrays |= dict(zip(keys, results)) if phase < 2 else {}
    moved = results[0].reshape(count, steps, pairs, size, lanes)

    pieces = exchange(moved)
    (updated,) = call(finish, [shape_of(*state.shape)], [state, pieces], [mixer])
    return (updated, residual)


def solution(mesh):
    in_specs = (P("tm", "space", None, None), P("space", None, None))
    out_specs = (P("tm", "space", None, None), P("tm", "space", None, None))
    return jax.shard_map(iteration, mesh=mesh, in_specs=in_specs, out_specs=out_specs, check_vma=False)
```

```python
import functools
import math

import jax
import jax.numpy as jnp
import numpy as np
from jax import lax
from jax.experimental import pallas as pl
from jax.experimental.pallas import tpu as pltpu
from jax.sharding import PartitionSpec as P


SWEEPS = 6
EARLY = 3

alpha_value = 0.1
time_step = 0.1
couple_first = 0.4
couple_cross = 0.05
reaction_shift = 0.1
relaxation = 0.9

SPLIT = 4
CHUNK = 8
LANES = 128
PAD = 8
EDGE = 12
MIB = 1024 * 1024


def reach(depth):
    return SWEEPS - max(depth, 0)


def ring(axis, step):
    count = lax.axis_size(axis)
    return [(i, (i + step) % count) for i in range(count)]


def hop(block, step):
    return lax.ppermute(block, "space", ring("space", step))


def low_mask(tile):
    return lax.broadcasted_iota(jnp.int32, tile.shape, tile.ndim - 1) % 2 == 0


def first_mask(tile):
    return lax.broadcasted_iota(jnp.int32, tile.shape, tile.ndim - 1) // 2 % 2 == 0


def turn(tile, step):
    return pltpu.roll(tile, step % tile.shape[-1], tile.ndim - 1)


def merge(low, high, low_at=0, high_at=1):
    low = turn(low, -1) if low_at else low
    high = high if high_at else turn(high, 1)
    return jnp.where(low_mask(low), low, high)


def swap(tile):
    return jnp.where(low_mask(tile), turn(tile, -1), turn(tile, 1))


def stage_tile(mix, stage):
    third = mix.shape[0] * LANES
    for part in range(mix.shape[0]):
        stage[PAD + part * LANES : PAD + (part + 1) * LANES] = mix[part].T
    stage[:PAD] = stage[third : third + PAD]
    stage[third + PAD :] = stage[PAD : 2 * PAD]


def layer_half(layer, width):
    return (layer, True) if 2 * layer < width else (width - 1 - layer, False)


def copy_in(sems, pairs):
    copies = [pltpu.make_async_copy(a, b, sems.at[i]) for i, (a, b) in enumerate(pairs)]
    for copy in copies:
        copy.start()
    return copies


def split(source, target, step):
    some = source.shape[0] // SPLIT
    return [
        (source.at[pl.ds(i * some, some), step], target.at[pl.ds(i * some, some), step])
        for i in range(SPLIT)
    ]


def pack_own(
    position, state_hbm, initial_hbm, out_hbm, first_hbm, up, down, state, initial, out, first, stage, mix, sems, out_sems
):
    count, steps = out.shape[:2]
    width, second, third = state.shape[1:]
    size = third // count
    pairs = width // 2
    rows = size + 2 * SWEEPS
    parts = third // LANES
    loads = []
    for pair in range(pairs):
        for i, layer in enumerate((pair, width - 1 - pair)):
            loads += copy_in(
                sems.at[pl.ds(4 * pair + 2 * i, 2)],
                [(state_hbm.at[:, layer], state.at[:, layer]), (initial_hbm.at[layer], initial.at[layer])],
            )
    stores = []
    for pair in range(pairs):
        for load in loads[4 * pair : 4 * pair + 4]:
            load.wait()
        for step in range(steps + 1):
            slot = step % 2
            for part in range(parts):
                here = slice(part * LANES, (part + 1) * LANES)
                for half, layer in enumerate((pair, width - 1 - pair)):
                    source = state[step, layer, :, here] if step < steps else initial[layer, :, here]
                    mix[slot, part, pl.ds(half, second, stride=2), :] = source
            stage_tile(mix.at[slot], stage.at[slot])
            if step < steps:
                for b in range(count):
                    begin = PAD - SWEEPS + b * size
                    out[b, step, pair * rows : (pair + 1) * rows] = stage[slot, begin : begin + rows]
            else:
                begin = pl.multiple_of(position[0] * size, 8)
                first[pair] = stage[slot, pl.ds(begin, size + 2 * PAD), :]
        if pair % 2:
            here = pl.ds((pair - 1) * rows, 2 * rows)
            stores += copy_in(
                out_sems.at[pl.ds(pair // 2, 1)],
                [(out.at[:, :, here], out_hbm.at[:, :, here])],
            )
    stores += copy_in(out_sems.at[pl.ds(pairs // 2, 1)], [(first, first_hbm)])
    at = 0
    for step in range(steps):
        for j in range(EARLY):
            for part in range(parts):
                here = slice(part * LANES, (part + 1) * LANES)
                up[at : at + second] = state[step, width - EARLY + j, :, here]
                down[at : at + second] = state[step, j, :, here]
                at += second
    short = size + 2 * (SWEEPS - 2)
    begin = PAD - SWEEPS + 2
    for slot in range(SWEEPS // 2):
        for out_ref, layers in (
            (up, [width - a for a in (2 * slot + 1, 2 * slot + 2)]),
            (down, [a - 1 for a in (2 * slot + 1, 2 * slot + 2)]),
        ):
            (one, one_low), (two, two_low) = [layer_half(layer, width) for layer in layers]
            out_ref[at : at + short] = merge(
                first[one, begin : begin + short],
                first[two, begin : begin + short],
                0 if one_low else 1,
                0 if two_low else 1,
            )
        at += short
    for store in stores:
        store.wait()


def early_rows(size):
    return [size + 2 * reach(EARLY - j) for j in range(EARLY)]


def late_rows(size):
    return [size + 2 * reach(SWEEPS - j) for j in range(SWEEPS - EARLY)]


def offsets(sizes):
    return [sum(sizes[:i]) for i in range(len(sizes))]


def pack_early(after, lower, upper, out_hbm, kept_low, kept_high, out, stage, mix, sems):
    count, steps = out.shape[:2]
    parts = mix.shape[1]
    second = mix.shape[2] // 2
    size = parts * LANES // count
    sizes = early_rows(size)
    layer = parts * second
    raw = EARLY * steps * layer
    stores = []
    for i, (source, target, nearest) in enumerate(
        ((lower, kept_low, EARLY - 1), (upper, kept_high, 0))
    ):
        pieces = [
            (source.at[pl.ds((step * EARLY + nearest) * layer, layer)], target.at[pl.ds(step * layer, layer)])
            for step in range(steps)
        ]
        rest = source.shape[0] - raw
        pieces.append((source.at[pl.ds(raw, rest)], target.at[pl.ds(steps * layer, rest)]))
        stores += copy_in(sems.at[pl.ds(i * (steps + 1), steps + 1)], pieces)
    for step in range(steps):
        for j, (rows, at) in enumerate(zip(sizes, offsets(sizes))):
            slot = j % 2
            for part in range(parts):
                low = ((step * EARLY + j) * parts + part) * second
                high = ((step * EARLY + EARLY - 1 - j) * parts + part) * second
                mix[slot, part, pl.ds(0, second, stride=2), :] = lower[low : low + second]
                mix[slot, part, pl.ds(1, second, stride=2), :] = upper[high : high + second]
            stage_tile(mix.at[slot], stage.at[slot])
            for b in range(count):
                begin = PAD - (rows - size) // 2 + b * size
                out[b, step, at : at + rows] = stage[slot, begin : begin + rows]
        stores += copy_in(
            sems.at[pl.ds(2 * steps + 2 + step * SPLIT, SPLIT)], split(out, out_hbm, step)
        )
    for store in stores:
        store.wait()


def pack_late(pairs, size, own, up, down):
    horizon = own.shape[0]
    half = horizon // 2
    width = 2 * pairs
    stride = size + 2 * SWEEPS
    at = 0
    for j, rows in enumerate(late_rows(size)):
        a = SWEEPS - j
        for t in range(half):
            for out, layer in ((up, width - a), (down, a - 1)):
                pair, low = layer_half(layer, width)
                begin = pair * stride + (stride - rows) // 2
                before = own[t, begin : begin + rows]
                after = own[t + half, begin : begin + rows]
                here = 0 if low else 1
                out[at : at + rows] = merge(before, after, here, here)
            at += rows


def real_forward(values):
    count = len(values)
    if count == 1:
        return [(values[0], None)]
    if count == 2:
        return [(values[0] + values[1], None), (values[0] - values[1], None)]
    even = real_forward(values[0::2])
    odd = real_forward(values[1::2])
    half = count // 2
    result = [None] * (half + 1)
    for k in range(count // 4 + 1):
        even_real, even_imag = even[k]
        odd_real, odd_imag = odd[k]
        if k == 0:
            result[0] = (even_real + odd_real, None)
            result[half] = (even_real - odd_real, None)
        elif 4 * k == count:
            result[k] = (even_real, -odd_real)
        else:
            cos, sin = math.cos(2 * math.pi * k / count), math.sin(2 * math.pi * k / count)
            if odd_imag is None:
                turned_real, turned_imag = cos * odd_real, -sin * odd_real
            else:
                turned_real = cos * odd_real + sin * odd_imag
                turned_imag = cos * odd_imag - sin * odd_real
            if even_imag is None:
                result[k] = (even_real + turned_real, turned_imag)
                result[half - k] = (even_real - turned_real, turned_imag)
            else:
                result[k] = (even_real + turned_real, even_imag + turned_imag)
                result[half - k] = (even_real - turned_real, turned_imag - even_imag)
    return result


def real_inverse(modes):
    half = len(modes) - 1
    count = 2 * half
    if count == 2:
        return [modes[0][0] + modes[1][0], modes[0][0] - modes[1][0]]
    even, odd = [], []
    for k in range(count // 4 + 1):
        real, imag = modes[k]
        other_real, other_imag = modes[half - k]
        if k == 0:
            even.append((real + other_real, None))
            odd.append((real - other_real, None))
        elif 4 * k == count:
            even.append((2.0 * real, None))
            odd.append((-2.0 * imag, None))
        else:
            cos, sin = math.cos(2 * math.pi * k / count), math.sin(2 * math.pi * k / count)
            even.append((real + other_real, imag - other_imag))
            minus_real, minus_imag = real - other_real, imag + other_imag
            odd.append((cos * minus_real - sin * minus_imag, sin * minus_real + cos * minus_imag))
    result = [None] * count
    result[0::2] = real_inverse(even)
    result[1::2] = real_inverse(odd)
    return result


def mode_inverses(horizon):
    rho = alpha_value ** (1.0 / horizon)
    angles = 2.0 * math.pi * np.arange(horizon // 2 + 1) / horizon
    shift = (
        1.0 + reaction_shift + 2.0 * couple_first + 4.0 * couple_cross - rho * np.cos(angles)
    ) + 1j * rho * np.sin(angles)
    return 1.0 / shift


def sweep_table(horizon, lanes):
    inverse = relaxation * mode_inverses(horizon)
    rows = [(inverse[0].real, 0.0, 0.0, inverse[-1].real)]
    rows += [(v.real, -v.imag, v.imag, v.real) for v in inverse[1:-1]]
    table = couple_cross * np.array(rows)
    quarter = horizon // 4
    mode = np.arange(quarter)[:, None] + quarter * (np.arange(lanes) // 2 % 2)[None, :]
    spread = np.moveaxis(table[mode], -1, 1)[:, :, None, :]
    return np.broadcast_to(spread, (quarter, 4, 8, lanes)).astype(np.float32)


class Plan:
    def __init__(self, pairs):
        self.last = SWEEPS + pairs - 1
        self.begins = [SWEEPS, 0]
        self.final = len(self.begins) - 1

    def fresh(self, phase):
        end = self.last if phase == 0 else self.begins[phase - 1]
        return range(self.begins[phase] + 1, end + 1)

    def rows(self, phase, level):
        fresh = self.fresh(phase)
        return range(fresh.start + level, min(fresh.stop - 1 + level, self.last) + 1)

    def arrays(self, phase):
        return [(phase, level) for level in range(SWEEPS) if self.rows(phase, level)]

    def find(self, phase, level, row):
        for p in range(phase, -1, -1):
            if row in self.rows(p, level):
                return (p, level), row - self.rows(p, level).start
        raise ValueError((phase, level, row))

    def needed(self, phase):
        keys = set()
        for level in range(1, SWEEPS):
            for row in self.rows(phase, level):
                keys.add(self.find(phase, 0, row)[0])
                for x in (row - 1, row, min(row + 1, self.last)):
                    keys.add(self.find(phase, level - 1, x)[0])
        if phase == self.final:
            for row in range(SWEEPS, self.last + 1):
                keys.add(self.find(phase, SWEEPS - 1, row)[0])
        return sorted(k for k in keys if k[0] < phase)

    def shape(self, key, horizon, size, lanes):
        rows = size + 2 * EDGE
        return (horizon, len(self.rows(*key)), rows, lanes)


def loop(count, copies, step):
    while count % copies:
        copies -= 1

    def several(index, carry):
        for i in range(copies):
            step(index * copies + i, 0)
        return carry

    lax.fori_loop(0, count // copies, several, 0)


def second_sum(tile):
    return turn(tile, 2) + turn(tile, -2)


def solve(phase, plan, pairs, size, names, far, *refs):
    named = dict(zip(names, refs))
    outs = refs[len(names) :]
    state, weighted, sems = refs[-3:]
    near = refs[-3 - len(far) : -3]
    halo = (SWEEPS // 2) * (size + 2 * (SWEEPS - 2))
    sources = {}
    for name in far:
        sources[name] = named[name]
        if name in ("first_low", "first_high"):
            sources[name] = named[name].at[pl.ds(named[name].shape[0] - halo, halo)]
    loads = dict(zip(far, copy_in(sems, [(sources[n], r) for n, r in zip(far, near)])))
    named |= dict(zip(far, near))
    horizon = weighted.shape[0]
    half, quarter = horizon // 2, horizon // 4
    last = plan.last
    window = size + 2 * EDGE
    at = PAD
    fresh = plan.fresh(phase)
    held = range(fresh.start - 1, fresh.stop + 1)
    keys = plan.arrays(phase)
    count = len(keys)
    ends = phase == plan.final
    results = outs[:1] if ends else outs[:count]
    inner_refs = refs[len(names) + len(results) :][:count] if ends or phase == 0 else results
    final = refs[len(names) + 1 + count] if ends else None
    arrays = dict(zip(keys, inner_refs))
    for key in plan.needed(phase):
        arrays[key] = named[key]

    own, early, first = named["own"], named.get("early"), named["first"]
    early_sizes, late_sizes = early_rows(size), late_rows(size)
    early_at, late_at = offsets(early_sizes), offsets([half * rows for rows in late_sizes])
    late_count = SWEEPS - EARLY
    own_rows = size + 2 * SWEEPS

    def fill(t, carry):
        for x in held:
            if x > last:
                continue
            if x >= SWEEPS:
                begin = at + EDGE - SWEEPS
                state[1 + t, x - held.start, begin : begin + own_rows] = own[
                    t, (x - SWEEPS) * own_rows : (x - SWEEPS + 1) * own_rows
                ]
            elif x >= late_count:
                j = x - late_count
                begin = at + EDGE - (early_sizes[j] - size) // 2
                state[1 + t, x - held.start, begin : begin + early_sizes[j]] = early[
                    t, early_at[j] : early_at[j] + early_sizes[j]
                ]
        return carry

    loop(horizon, 4, fill)
    for x in held:
        if x < late_count:
            rows, where = late_sizes[x], late_at[x]
            begin = at + EDGE - (rows - size) // 2
            for t in range(half):
                low = named["late_low"][where + t * rows : where + (t + 1) * rows]
                high = named["late_high"][where + t * rows : where + (t + 1) * rows]
                state[1 + t, x - held.start, begin : begin + rows] = merge(low, high, 0, 0)
                state[1 + half + t, x - held.start, begin : begin + rows] = merge(low, high, 1, 1)
    for name in ("first", "first_low", "first_high"):
        if name in loads:
            loads.pop(name).wait()
    for x in fresh:
        if x >= SWEEPS:
            begin = at + EDGE - PAD
            state[0, x - held.start, begin : begin + size + 2 * PAD] = first[x - SWEEPS]
        else:
            a = SWEEPS - x
            rows = size + 2 * (SWEEPS - 2)
            total = named["first_low"].shape[0]
            where = total - (SWEEPS // 2 - (a - 1) // 2) * rows
            low, high = named["first_low"][where : where + rows], named["first_high"][where : where + rows]
            slot = (a - 1) % 2
            tile = merge(low, high, slot, slot)
            begin = at + EDGE - SWEEPS + 2
            state[0, x - held.start, begin : begin + rows] = tile

    def weigh(t, carry):
        centre = time_step - 1.0 - 2.0 * couple_first - 4.0 * couple_cross
        for i in range(len(fresh)):
            for r in range(at, at + window, CHUNK):
                s = state[t + 1, i + 1, r : r + CHUNK]
                outer = state[t + 1, i, r : r + CHUNK]
                along = outer + (swap(s) if fresh[i] == last else state[t + 1, i + 2, r : r + CHUNK])
                across = (
                    state[t + 1, i + 1, r - 1 : r + CHUNK - 1]
                    + state[t + 1, i + 1, r + 1 : r + CHUNK + 1]
                    + second_sum(s)
                )
                weighted[t, i, r - at : r - at + CHUNK] = (
                    (state[t, i + 1, r : r + CHUNK] + couple_first * along)
                    + (couple_cross * across + s * (centre - time_step * (s * s)))
                )
        return carry

    loop(horizon, 8, weigh)

    inverses = mode_inverses(horizon)
    weights = [alpha_value ** (n / horizon) for n in range(horizon)]
    tiles = window // 8
    base = arrays[(phase, 0)]

    def transform(index, carry):
        i = index // tiles
        r = pl.ds(pl.multiple_of((index % tiles) * 8, 8), 8)
        spectrum = real_forward([weights[n] * weighted[n, i, r, :] for n in range(horizon)])
        reals, imags = [None] * half, [None] * half
        for k, (real, imag) in enumerate(spectrum):
            c = relaxation * inverses[k]
            if k == 0:
                reals[0] = float(c.real) * real
            elif k == half:
                imags[0] = float(c.real) * real
            else:
                reals[k] = float(c.real) * real - float(c.imag) * imag
                imags[k] = float(c.imag) * real + float(c.real) * imag
        for part, values in enumerate((reals, imags)):
            for k in range(quarter):
                one, two = values[k], values[k + quarter]
                mask = first_mask(one)
                base[part * half + 2 * k, i, r, :] = jnp.where(mask, one, turn(two, 2))
                base[part * half + 2 * k + 1, i, r, :] = jnp.where(mask, turn(one, -2), two)
        return carry

    loop(len(fresh) * tiles, 7, transform)

    table = named["table"]
    for load in loads.values():
        load.wait()

    def sweep(level):
        rows = plan.rows(phase, level)
        span = size + PAD
        begin = EDGE - PAD // 2
        target = arrays[(phase, level)]

        def read(level_, part, k, parity, x, r):
            key, i = plan.find(phase, level_, x)
            return arrays[key][part * half + 2 * k + parity, i, r : r + CHUNK]

        def mode(k, carry):
            a, b, c, d = [table[k, i] for i in range(4)]
            for x in rows:
                for r in range(begin, begin + span, CHUNK):
                    for parity in (0, 1):
                        near = []
                        for part in (0, 1):
                            v = read(level - 1, part, k, parity, x, r)
                            other = read(level - 1, part, k, 1 - parity, x, r)
                            inner = (
                                swap(v)
                                if x == last
                                else read(level - 1, part, k, parity, x + 1, r)
                            )
                            along = read(level - 1, part, k, parity, x - 1, r) + inner
                            across = (
                                read(level - 1, part, k, parity, x, r - 1)
                                + read(level - 1, part, k, parity, x, r + 1)
                            ) + (other + turn(other, 4 if parity == 0 else -4))
                            near.append(
                                (
                                    read(0, part, k, parity, x, r) + (1.0 - relaxation) * v,
                                    (couple_first / couple_cross) * along + across,
                                )
                            )
                        (rest_real, near_real), (rest_imag, near_imag) = near
                        values = (
                            rest_real + (a * near_real + b * near_imag),
                            rest_imag + (c * near_real + d * near_imag),
                        )
                        here = slice(r, r + CHUNK)
                        for part, value in enumerate(values):
                            m = part * half + 2 * k + parity
                            target[m, x - rows.start, here] = value
            return carry

        loop(quarter, 4, mode)

    for key in keys:
        if key[1]:
            sweep(key[1])
    if phase == 0:
        for store in copy_in(sems, [(arrays[key], ref) for key, ref in zip(keys, results)]):
            store.wait()
    if not ends:
        return

    kept = size // 8
    done = [plan.find(phase, SWEEPS - 1, SWEEPS + i) for i in range(pairs)]
    stores = []
    for i, (key, row) in enumerate(done):

        for index in range(kept):
            source = arrays[key]
            r = slice(EDGE + index * 8, EDGE + index * 8 + 8)
            parts = []
            for part in (0, 1):
                values = [None] * half
                for k in range(quarter):
                    even = source[part * half + 2 * k, row, r, :]
                    odd = source[part * half + 2 * k + 1, row, r, :]
                    mask = first_mask(even)
                    values[k] = jnp.where(mask, even, turn(odd, 2))
                    values[k + quarter] = jnp.where(mask, turn(even, -2), odd)
                parts.append(values)
            reals, imags = parts
            modes = [(reals[0], None)] + list(zip(reals[1:], imags[1:])) + [(imags[0], None)]
            for n, value in enumerate(real_inverse(modes)):
                final[n, i, index * 8 : index * 8 + 8] = (1.0 / (horizon * weights[n])) * value
        stores += copy_in(sems.at[pl.ds(i, 1)], [(final.at[:, i], results[0].at[:, i])])
    for store in stores:
        store.wait()


def finish(state, pieces, out, updated, mix, sems):
    count, steps, pairs, size, lanes = pieces.shape
    width = 2 * pairs
    second = lanes // 2
    per = LANES // size
    stores = []
    for step in range(steps):
        for pair in range(pairs):
            mirror = width - 1 - pair
            for part in range(count // per):
                here = slice(part * LANES, (part + 1) * LANES)
                piece = mix.at[pair % 2, part]
                piece[...] = jnp.concatenate(
                    [pieces[part * per + b, step, pair] for b in range(per)], axis=0
                ).T
                low, high = piece[pl.ds(0, second, stride=2), :], piece[pl.ds(1, second, stride=2), :]
                updated[step, pair, :, here] = state[step, pair, :, here] + low
                updated[step, mirror, :, here] = state[step, mirror, :, here] + high
            first = 2 * (step * pairs + pair)
            stores += copy_in(
                sems.at[pl.ds(first, 2)],
                [(updated.at[step, layer], out.at[step, layer]) for layer in (pair, mirror)],
            )
    for store in stores:
        store.wait()


def residual_of(state, carried, lower_hbm, upper_hbm, out, lower, upper, sems):
    steps, width, second, third = state.shape
    parts = third // LANES
    used = pl.ds(0, lower.shape[0])
    loads = copy_in(sems, [(lower_hbm.at[used], lower), (upper_hbm.at[used], upper)])
    for load in loads:
        load.wait()

    def outside(ref, step):
        at = step * parts * second
        return jnp.concatenate(
            [ref[at + part * second : at + (part + 1) * second] for part in range(parts)], axis=1
        )

    for step in range(steps):
        for layer in range(width):
            s = state[step, layer]
            below = outside(lower, step) if layer == 0 else state[step, layer - 1]
            above = outside(upper, step) if layer == width - 1 else state[step, layer + 1]
            before = carried[layer] if step == 0 else state[step - 1, layer]
            across = (
                pltpu.roll(s, 1, 0)
                + pltpu.roll(s, s.shape[0] - 1, 0)
                + pltpu.roll(s, 1, 1)
                + pltpu.roll(s, s.shape[1] - 1, 1)
            )
            centre = time_step - 1.0 - 2.0 * couple_first - 4.0 * couple_cross
            out[step, layer] = (
                (before + couple_first * (below + above))
                + (couple_cross * across + s * (centre - time_step * (s * s)))
            )


def shape_of(*dims):
    return jax.ShapeDtypeStruct(dims, jnp.float32)


def padded_bytes(shape):
    *major, rows, lanes = (1, 1, *shape)
    return 4 * math.prod(major) * (-(-rows // 8) * 8) * (-(-lanes // 128) * 128)


def call(kernel, outs, args, scratch=(), flops=2e6, scalars=0, far=(), far_outs=()):
    spaces = [
        pltpu.SMEM if i < scalars else pltpu.HBM if i in far else pltpu.VMEM for i in range(len(args))
    ]
    out_spaces = [pltpu.HBM if i in far_outs else pltpu.VMEM for i in range(len(outs))]
    held = [a.shape for i, a in enumerate(args) if i not in far]
    held += [o.shape for i, o in enumerate(outs) if i not in far_outs]
    held += [r.shape for r in scratch if len(r.shape) > 1]
    moved = sum(padded_bytes(a.shape) for a in (*args, *outs))
    args = [
        pltpu.with_memory_space_constraint(a, pltpu.HBM) if i in far else a for i, a in enumerate(args)
    ]
    outs = [pltpu.HBM(o.shape, o.dtype) if i in far_outs else o for i, o in enumerate(outs)]
    return pl.pallas_call(
        kernel,
        out_shape=tuple(outs),
        in_specs=[pl.BlockSpec(memory_space=space) for space in spaces],
        out_specs=tuple(pl.BlockSpec(memory_space=space) for space in out_spaces),
        scratch_shapes=list(scratch),
        compiler_params=pltpu.CompilerParams(
            vmem_limit_bytes=sum(padded_bytes(s) for s in held) + 2 * MIB
        ),
        cost_estimate=pl.CostEstimate(
            flops=int(flops), bytes_accessed=int(moved), transcendentals=0
        ),
    )(*args)


def vmem(*shape):
    return pltpu.VMEM(shape, jnp.float32)


def semaphores(count):
    return pltpu.SemaphoreType.DMA((count,))


def exchange(block):
    return lax.all_to_all(block, "tm", split_axis=0, concat_axis=0, tiled=True)


def iteration(state, initial):
    steps, width, second, third = state.shape
    count = lax.axis_size("tm")
    horizon = steps * count
    half = horizon // 2
    position = lax.axis_index("tm")
    pairs = width // 2
    size = third // count
    lanes = 2 * second
    stage = vmem(2, third + 2 * PAD, lanes)
    mixer = vmem(2, third // LANES, lanes, LANES)

    raw_rows = EARLY * steps * second * (third // LANES)
    sent_rows = raw_rows + (SWEEPS // 2) * (size + 2 * SWEEPS - 4)
    own_shape = (count, steps, pairs * (size + 2 * SWEEPS), lanes)
    first_shape = (pairs, size + 2 * PAD, lanes)
    sent, first, up, down = call(
        pack_own,
        [
            shape_of(*own_shape),
            shape_of(*first_shape),
            shape_of(sent_rows, LANES),
            shape_of(sent_rows, LANES),
        ],
        [position.reshape(1), state, initial],
        [
            vmem(*state.shape),
            vmem(*initial.shape),
            vmem(*own_shape),
            vmem(*first_shape),
            stage,
            mixer,
            semaphores(4 * pairs),
            semaphores(pairs // 2 + 1),
        ],
        scalars=1,
        far=(1, 2),
        far_outs=(0, 1),
    )
    own = exchange(sent).reshape(horizon, -1, lanes)

    lower = hop(up, 1)
    upper = hop(down, -1)

    late_shape = shape_of(half * sum(late_rows(size)), lanes)
    late_up, late_down = call(functools.partial(pack_late, pairs, size), [late_shape] * 2, [own])
    late_low = hop(late_up, 1)
    late_high = hop(late_down, -1)

    early_shape = (count, steps, sum(early_rows(size)), lanes)
    kept = shape_of(steps * second * (third // LANES) + sent_rows - raw_rows, LANES)
    sent_early, kept_low, kept_high = call(
        pack_early,
        [shape_of(*early_shape), kept, kept],
        [late_up, lower, upper],
        [vmem(*early_shape), stage, mixer, semaphores(2 * steps + 2 + SPLIT * steps)],
        far=(0,),
        far_outs=(0, 1, 2),
    )
    early = exchange(sent_early).reshape(horizon, -1, lanes)

    carried = lax.ppermute(state[steps - 1], "tm", [(i, i + 1) for i in range(count - 1)])
    carried = jnp.where(position == 0, initial, carried)
    (residual,) = call(
        residual_of,
        [shape_of(*state.shape)],
        [state, carried, kept_low, kept_high],
        [vmem(raw_rows // EARLY, LANES), vmem(raw_rows // EARLY, LANES), semaphores(2)],
        flops=6e6,
        far=(2, 3),
    )

    plan = Plan(pairs)
    table = jnp.asarray(sweep_table(horizon, lanes))
    arrays = {}
    for phase in range(plan.final + 1):
        ends = phase == plan.final
        inputs = {"table": table, "own": own, "first": first}
        if phase:
            inputs |= {"early": early, "first_low": kept_low, "first_high": kept_high}
        if ends:
            inputs |= {"late_low": late_low, "late_high": late_high}
        inputs |= {key: arrays[key] for key in plan.needed(phase)}
        keys = plan.arrays(phase)
        outs = [shape_of(*plan.shape(key, horizon, size, lanes)) for key in keys]
        fresh = len(plan.fresh(phase))
        halo = vmem((SWEEPS // 2) * (size + 2 * (SWEEPS - 2)), lanes)
        far = [n for n in inputs if n in ("first", "first_low", "first_high") or n[0] == 0]
        near = [halo if n[:6] == "first_" else vmem(*inputs[n].shape) for n in far]
        scratch = near + [
            vmem(horizon + 1, fresh + 2, size + 2 * EDGE + 2 * PAD, lanes),
            vmem(horizon, fresh, size + 2 * EDGE, lanes),
            semaphores(max(len(far), len(keys), pairs)),
        ]
        inner = [vmem(*o.shape) for o in outs]
        if phase == 0:
            scratch = inner + scratch
        if ends:
            scratch = inner + [vmem(horizon, pairs, size, lanes)] + scratch
            outs = [shape_of(horizon, pairs, size, lanes)]
        results = call(
            functools.partial(solve, phase, plan, pairs, size, list(inputs), far),
            outs,
            list(inputs.values()),
            scratch,
            flops=3e7,
            far=[i for i, n in enumerate(inputs) if n in far],
            far_outs=range(len(outs)) if ends or phase == 0 else (),
        )
        arrays |= {} if ends else dict(zip(keys, results))
    moved = results[0].reshape(count, steps, pairs, size, lanes)

    pieces = exchange(moved)
    (updated,) = call(
        finish,
        [shape_of(*state.shape)],
        [state, pieces],
        [vmem(*state.shape), mixer, semaphores(steps * width)],
        far_outs=(0,),
    )
    return (updated, residual)


def solution(mesh):
    in_specs = (P("tm", "space", None, None), P("space", None, None))
    out_specs = (P("tm", "space", None, None), P("tm", "space", None, None))
    return jax.shard_map(iteration, mesh=mesh, in_specs=in_specs, out_specs=out_specs, check_vma=False)
```

```python
import functools
import math

import jax
import jax.numpy as jnp
import numpy as np
from jax import lax
from jax.experimental import pallas as pl
from jax.experimental.pallas import tpu as pltpu
from jax.sharding import PartitionSpec as P


SWEEPS = 6
EARLY = 3

alpha_value = 0.1
time_step = 0.1
couple_first = 0.4
couple_cross = 0.05
reaction_shift = 0.1
relaxation = 0.9

SPLIT = 4
CHUNK = 8
LANES = 128
PAD = 8
EDGE = 12
MIB = 1024 * 1024


def reach(depth):
    return SWEEPS - max(depth, 0)


def ring(axis, step):
    count = lax.axis_size(axis)
    return [(i, (i + step) % count) for i in range(count)]


def hop(block, step):
    return lax.ppermute(block, "space", ring("space", step))


def low_mask(tile):
    return lax.broadcasted_iota(jnp.int32, tile.shape, tile.ndim - 1) % 2 == 0


def first_mask(tile):
    return lax.broadcasted_iota(jnp.int32, tile.shape, tile.ndim - 1) // 2 % 2 == 0


def turn(tile, step):
    return pltpu.roll(tile, step % tile.shape[-1], tile.ndim - 1)


def merge(low, high, low_at=0, high_at=1):
    low = turn(low, -1) if low_at else low
    high = high if high_at else turn(high, 1)
    return jnp.where(low_mask(low), low, high)


def swap(tile):
    return jnp.where(low_mask(tile), turn(tile, -1), turn(tile, 1))


def stage_tile(mix, stage):
    third = mix.shape[0] * LANES
    for part in range(mix.shape[0]):
        stage[PAD + part * LANES : PAD + (part + 1) * LANES] = mix[part].T
    stage[:PAD] = stage[third : third + PAD]
    stage[third + PAD :] = stage[PAD : 2 * PAD]


def layer_half(layer, width):
    return (layer, True) if 2 * layer < width else (width - 1 - layer, False)


def copy_in(sems, pairs):
    copies = [pltpu.make_async_copy(a, b, sems.at[i]) for i, (a, b) in enumerate(pairs)]
    for copy in copies:
        copy.start()
    return copies


def split(source, target, step):
    some = source.shape[0] // SPLIT
    return [
        (source.at[pl.ds(i * some, some), step], target.at[pl.ds(i * some, some), step])
        for i in range(SPLIT)
    ]


def pack_own(
    position,
    state_hbm,
    initial_hbm,
    out_hbm,
    first_hbm,
    up_hbm,
    down_hbm,
    state,
    initial,
    out,
    first,
    up,
    down,
    stage,
    mix,
    sems,
    out_sems,
    halo_sems,
):
    count, steps = out.shape[:2]
    width, second, third = state.shape[1:]
    size = third // count
    pairs = width // 2
    rows = size + 2 * SWEEPS
    parts = third // LANES
    loads = []
    for pair in range(pairs):
        for i, layer in enumerate((pair, width - 1 - pair)):
            loads += copy_in(
                sems.at[pl.ds(4 * pair + 2 * i, 2)],
                [(state_hbm.at[:, layer], state.at[:, layer]), (initial_hbm.at[layer], initial.at[layer])],
            )
    stores = []
    for pair in range(pairs):
        for load in loads[4 * pair : 4 * pair + 4]:
            load.wait()
        if pair < EARLY:
            pieces = []
            for step in range(steps):
                for part in range(parts):
                    here = pl.ds(part * LANES, LANES)
                    for target, layer, j in (
                        (up_hbm, width - 1 - pair, EARLY - 1 - pair),
                        (down_hbm, pair, pair),
                    ):
                        row = ((step * EARLY + j) * parts + part) * second
                        pieces.append((state.at[step, layer, :, here], target.at[pl.ds(row, second)]))
            stores += copy_in(halo_sems.at[pl.ds(pair * len(pieces), len(pieces))], pieces)
        for step in range(steps + 1):
            slot = step % 2
            for part in range(parts):
                here = slice(part * LANES, (part + 1) * LANES)
                for half, layer in enumerate((pair, width - 1 - pair)):
                    source = state[step, layer, :, here] if step < steps else initial[layer, :, here]
                    mix[slot, part, pl.ds(half, second, stride=2), :] = source
            stage_tile(mix.at[slot], stage.at[slot])
            if step < steps:
                for b in range(count):
                    begin = PAD - SWEEPS + b * size
                    out[b, step, pair * rows : (pair + 1) * rows] = stage[slot, begin : begin + rows]
            else:
                begin = pl.multiple_of(position[0] * size, 8)
                first[pair] = stage[slot, pl.ds(begin, size + 2 * PAD), :]
        if pair % 2:
            here = pl.ds((pair - 1) * rows, 2 * rows)
            stores += copy_in(
                out_sems.at[pl.ds(pair // 2, 1)],
                [(out.at[:, :, here], out_hbm.at[:, :, here])],
            )
    stores += copy_in(out_sems.at[pl.ds(pairs // 2, 1)], [(first, first_hbm)])
    at = 0
    short = size + 2 * (SWEEPS - 2)
    begin = PAD - SWEEPS + 2
    for slot in range(SWEEPS // 2):
        for out_ref, layers in (
            (up, [width - a for a in (2 * slot + 1, 2 * slot + 2)]),
            (down, [a - 1 for a in (2 * slot + 1, 2 * slot + 2)]),
        ):
            (one, one_low), (two, two_low) = [layer_half(layer, width) for layer in layers]
            out_ref[at : at + short] = merge(
                first[one, begin : begin + short],
                first[two, begin : begin + short],
                0 if one_low else 1,
                0 if two_low else 1,
            )
        at += short
    raw = up_hbm.shape[0] - at
    stores += copy_in(
        halo_sems.at[pl.ds(2 * EARLY * steps * parts, 2)],
        [(up, up_hbm.at[pl.ds(raw, at)]), (down, down_hbm.at[pl.ds(raw, at)])],
    )
    for store in stores:
        store.wait()


def early_rows(size):
    return [size + 2 * reach(EARLY - j) for j in range(EARLY)]


def late_rows(size):
    return [size + 2 * reach(SWEEPS - j) for j in range(SWEEPS - EARLY)]


def offsets(sizes):
    return [sum(sizes[:i]) for i in range(len(sizes))]


def pack_early(after, lower, upper, out_hbm, kept_low, kept_high, out, stage, mix, sems):
    count, steps = out.shape[:2]
    parts = mix.shape[1]
    second = mix.shape[2] // 2
    size = parts * LANES // count
    sizes = early_rows(size)
    layer = parts * second
    raw = EARLY * steps * layer
    stores = []
    for i, (source, target, nearest) in enumerate(
        ((lower, kept_low, EARLY - 1), (upper, kept_high, 0))
    ):
        pieces = [
            (source.at[pl.ds((step * EARLY + nearest) * layer, layer)], target.at[pl.ds(step * layer, layer)])
            for step in range(steps)
        ]
        rest = source.shape[0] - raw
        pieces.append((source.at[pl.ds(raw, rest)], target.at[pl.ds(steps * layer, rest)]))
        stores += copy_in(sems.at[pl.ds(i * (steps + 1), steps + 1)], pieces)
    for step in range(steps):
        for j, (rows, at) in enumerate(zip(sizes, offsets(sizes))):
            slot = j % 2
            for part in range(parts):
                low = ((step * EARLY + j) * parts + part) * second
                high = ((step * EARLY + EARLY - 1 - j) * parts + part) * second
                mix[slot, part, pl.ds(0, second, stride=2), :] = lower[low : low + second]
                mix[slot, part, pl.ds(1, second, stride=2), :] = upper[high : high + second]
            stage_tile(mix.at[slot], stage.at[slot])
            for b in range(count):
                begin = PAD - (rows - size) // 2 + b * size
                out[b, step, at : at + rows] = stage[slot, begin : begin + rows]
        stores += copy_in(
            sems.at[pl.ds(2 * steps + 2 + step * SPLIT, SPLIT)], split(out, out_hbm, step)
        )
    for store in stores:
        store.wait()


def pack_late(pairs, size, own, up, down):
    horizon = own.shape[0]
    half = horizon // 2
    width = 2 * pairs
    stride = size + 2 * SWEEPS
    at = 0
    for j, rows in enumerate(late_rows(size)):
        a = SWEEPS - j
        for t in range(half):
            for out, layer in ((up, width - a), (down, a - 1)):
                pair, low = layer_half(layer, width)
                begin = pair * stride + (stride - rows) // 2
                before = own[t, begin : begin + rows]
                after = own[t + half, begin : begin + rows]
                here = 0 if low else 1
                out[at : at + rows] = merge(before, after, here, here)
            at += rows


def real_forward(values):
    count = len(values)
    if count == 1:
        return [(values[0], None)]
    if count == 2:
        return [(values[0] + values[1], None), (values[0] - values[1], None)]
    even = real_forward(values[0::2])
    odd = real_forward(values[1::2])
    half = count // 2
    result = [None] * (half + 1)
    for k in range(count // 4 + 1):
        even_real, even_imag = even[k]
        odd_real, odd_imag = odd[k]
        if k == 0:
            result[0] = (even_real + odd_real, None)
            result[half] = (even_real - odd_real, None)
        elif 4 * k == count:
            result[k] = (even_real, -odd_real)
        else:
            cos, sin = math.cos(2 * math.pi * k / count), math.sin(2 * math.pi * k / count)
            if odd_imag is None:
                turned_real, turned_imag = cos * odd_real, -sin * odd_real
            else:
                turned_real = cos * odd_real + sin * odd_imag
                turned_imag = cos * odd_imag - sin * odd_real
            if even_imag is None:
                result[k] = (even_real + turned_real, turned_imag)
                result[half - k] = (even_real - turned_real, turned_imag)
            else:
                result[k] = (even_real + turned_real, even_imag + turned_imag)
                result[half - k] = (even_real - turned_real, turned_imag - even_imag)
    return result


def real_inverse(modes):
    half = len(modes) - 1
    count = 2 * half
    if count == 2:
        return [modes[0][0] + modes[1][0], modes[0][0] - modes[1][0]]
    even, odd = [], []
    for k in range(count // 4 + 1):
        real, imag = modes[k]
        other_real, other_imag = modes[half - k]
        if k == 0:
            even.append((real + other_real, None))
            odd.append((real - other_real, None))
        elif 4 * k == count:
            even.append((2.0 * real, None))
            odd.append((-2.0 * imag, None))
        else:
            cos, sin = math.cos(2 * math.pi * k / count), math.sin(2 * math.pi * k / count)
            even.append((real + other_real, imag - other_imag))
            minus_real, minus_imag = real - other_real, imag + other_imag
            odd.append((cos * minus_real - sin * minus_imag, sin * minus_real + cos * minus_imag))
    result = [None] * count
    result[0::2] = real_inverse(even)
    result[1::2] = real_inverse(odd)
    return result


def mode_inverses(horizon):
    rho = alpha_value ** (1.0 / horizon)
    angles = 2.0 * math.pi * np.arange(horizon // 2 + 1) / horizon
    shift = (
        1.0 + reaction_shift + 2.0 * couple_first + 4.0 * couple_cross - rho * np.cos(angles)
    ) + 1j * rho * np.sin(angles)
    return 1.0 / shift


def sweep_table(horizon, lanes):
    inverse = relaxation * mode_inverses(horizon)
    rows = [(inverse[0].real, 0.0, 0.0, inverse[-1].real)]
    rows += [(v.real, -v.imag, v.imag, v.real) for v in inverse[1:-1]]
    table = couple_cross * np.array(rows)
    quarter = horizon // 4
    mode = np.arange(quarter)[:, None] + quarter * (np.arange(lanes) // 2 % 2)[None, :]
    spread = np.moveaxis(table[mode], -1, 1)[:, :, None, :]
    return np.broadcast_to(spread, (quarter, 4, 8, lanes)).astype(np.float32)


FAR = ("late_low", "late_high", "first", "first_low", "first_high")


class Plan:
    def __init__(self, pairs):
        self.last = SWEEPS + pairs - 1
        self.begins = [SWEEPS, 0]
        self.final = len(self.begins) - 1

    def fresh(self, phase):
        end = self.last if phase == 0 else self.begins[phase - 1]
        return range(self.begins[phase] + 1, end + 1)

    def rows(self, phase, level):
        fresh = self.fresh(phase)
        return range(fresh.start + level, min(fresh.stop - 1 + level, self.last) + 1)

    def arrays(self, phase):
        return [(phase, level) for level in range(SWEEPS) if self.rows(phase, level)]

    def find(self, phase, level, row):
        for p in range(phase, -1, -1):
            if row in self.rows(p, level):
                return (p, level), row - self.rows(p, level).start
        raise ValueError((phase, level, row))

    def needed(self, phase):
        keys = set()
        for level in range(1, SWEEPS):
            for row in self.rows(phase, level):
                keys.add(self.find(phase, 0, row)[0])
                for x in (row - 1, row, min(row + 1, self.last)):
                    keys.add(self.find(phase, level - 1, x)[0])
        if phase == self.final:
            for row in range(SWEEPS, self.last + 1):
                keys.add(self.find(phase, SWEEPS - 1, row)[0])
        return sorted(k for k in keys if k[0] < phase)

    def shape(self, key, horizon, size, lanes):
        rows = size + 2 * EDGE
        return (horizon, len(self.rows(*key)), rows, lanes)


def loop(count, copies, step):
    while count % copies:
        copies -= 1

    def several(index, carry):
        for i in range(copies):
            step(index * copies + i, 0)
        return carry

    lax.fori_loop(0, count // copies, several, 0)


def second_sum(tile):
    return turn(tile, 2) + turn(tile, -2)


def solve(phase, plan, pairs, size, names, far, *refs):
    named = dict(zip(names, refs))
    outs = refs[len(names) :]
    state, weighted, sems = refs[-3:]
    near = refs[-3 - len(far) : -3]
    halo = (SWEEPS // 2) * (size + 2 * (SWEEPS - 2))
    sources = {}
    for name in far:
        sources[name] = named[name]
        if name in ("first_low", "first_high"):
            sources[name] = named[name].at[pl.ds(named[name].shape[0] - halo, halo)]
    loads = dict(zip(far, copy_in(sems, [(sources[n], r) for n, r in zip(far, near)])))
    named |= dict(zip(far, near))
    horizon = weighted.shape[0]
    half, quarter = horizon // 2, horizon // 4
    last = plan.last
    window = size + 2 * EDGE
    at = PAD
    fresh = plan.fresh(phase)
    held = range(fresh.start - 1, fresh.stop + 1)
    keys = plan.arrays(phase)
    count = len(keys)
    ends = phase == plan.final
    results = outs[:1] if ends else outs[:count]
    inner_refs = refs[len(names) + len(results) :][:count] if ends or phase == 0 else results
    final = refs[len(names) + 1 + count] if ends else None
    arrays = dict(zip(keys, inner_refs))
    for key in plan.needed(phase):
        arrays[key] = named[key]

    own, early, first = named["own"], named.get("early"), named["first"]
    early_sizes, late_sizes = early_rows(size), late_rows(size)
    early_at, late_at = offsets(early_sizes), offsets([half * rows for rows in late_sizes])
    late_count = SWEEPS - EARLY
    own_rows = size + 2 * SWEEPS

    def fill(t, carry):
        for x in held:
            if x > last:
                continue
            if x >= SWEEPS:
                begin = at + EDGE - SWEEPS
                state[1 + t, x - held.start, begin : begin + own_rows] = own[
                    t, (x - SWEEPS) * own_rows : (x - SWEEPS + 1) * own_rows
                ]
            elif x >= late_count:
                j = x - late_count
                begin = at + EDGE - (early_sizes[j] - size) // 2
                state[1 + t, x - held.start, begin : begin + early_sizes[j]] = early[
                    t, early_at[j] : early_at[j] + early_sizes[j]
                ]
        return carry

    loop(horizon, 4, fill)
    for name in FAR:
        if name in loads:
            loads.pop(name).wait()
    for x in held:
        if x < late_count:
            rows, where = late_sizes[x], late_at[x]
            begin = at + EDGE - (rows - size) // 2
            for t in range(half):
                low = named["late_low"][where + t * rows : where + (t + 1) * rows]
                high = named["late_high"][where + t * rows : where + (t + 1) * rows]
                state[1 + t, x - held.start, begin : begin + rows] = merge(low, high, 0, 0)
                state[1 + half + t, x - held.start, begin : begin + rows] = merge(low, high, 1, 1)
    for x in fresh:
        if x >= SWEEPS:
            begin = at + EDGE - PAD
            state[0, x - held.start, begin : begin + size + 2 * PAD] = first[x - SWEEPS]
        else:
            a = SWEEPS - x
            rows = size + 2 * (SWEEPS - 2)
            total = named["first_low"].shape[0]
            where = total - (SWEEPS // 2 - (a - 1) // 2) * rows
            low, high = named["first_low"][where : where + rows], named["first_high"][where : where + rows]
            slot = (a - 1) % 2
            tile = merge(low, high, slot, slot)
            begin = at + EDGE - SWEEPS + 2
            state[0, x - held.start, begin : begin + rows] = tile

    def weigh(t, carry):
        centre = time_step - 1.0 - 2.0 * couple_first - 4.0 * couple_cross
        for i in range(len(fresh)):
            for r in range(at, at + window, CHUNK):
                s = state[t + 1, i + 1, r : r + CHUNK]
                outer = state[t + 1, i, r : r + CHUNK]
                along = outer + (swap(s) if fresh[i] == last else state[t + 1, i + 2, r : r + CHUNK])
                across = (
                    state[t + 1, i + 1, r - 1 : r + CHUNK - 1]
                    + state[t + 1, i + 1, r + 1 : r + CHUNK + 1]
                    + second_sum(s)
                )
                weighted[t, i, r - at : r - at + CHUNK] = (
                    (state[t, i + 1, r : r + CHUNK] + couple_first * along)
                    + (couple_cross * across + s * (centre - time_step * (s * s)))
                )
        return carry

    loop(horizon, 8, weigh)

    inverses = mode_inverses(horizon)
    weights = [alpha_value ** (n / horizon) for n in range(horizon)]
    tiles = window // 8
    base = arrays[(phase, 0)]

    def transform(index, carry):
        i = index // tiles
        r = pl.ds(pl.multiple_of((index % tiles) * 8, 8), 8)
        spectrum = real_forward([weights[n] * weighted[n, i, r, :] for n in range(horizon)])
        reals, imags = [None] * half, [None] * half
        for k, (real, imag) in enumerate(spectrum):
            c = relaxation * inverses[k]
            if k == 0:
                reals[0] = float(c.real) * real
            elif k == half:
                imags[0] = float(c.real) * real
            else:
                reals[k] = float(c.real) * real - float(c.imag) * imag
                imags[k] = float(c.imag) * real + float(c.real) * imag
        for part, values in enumerate((reals, imags)):
            for k in range(quarter):
                one, two = values[k], values[k + quarter]
                mask = first_mask(one)
                base[part * half + 2 * k, i, r, :] = jnp.where(mask, one, turn(two, 2))
                base[part * half + 2 * k + 1, i, r, :] = jnp.where(mask, turn(one, -2), two)
        return carry

    loop(len(fresh) * tiles, 7, transform)

    table = named["table"]
    for load in loads.values():
        load.wait()

    def sweep(level):
        rows = plan.rows(phase, level)
        span = size + PAD
        begin = EDGE - PAD // 2
        target = arrays[(phase, level)]

        def read(level_, part, k, parity, x, r):
            key, i = plan.find(phase, level_, x)
            return arrays[key][part * half + 2 * k + parity, i, r : r + CHUNK]

        def mode(k, carry):
            a, b, c, d = [table[k, i] for i in range(4)]
            for x in rows:
                for r in range(begin, begin + span, CHUNK):
                    for parity in (0, 1):
                        near = []
                        for part in (0, 1):
                            v = read(level - 1, part, k, parity, x, r)
                            other = read(level - 1, part, k, 1 - parity, x, r)
                            inner = (
                                swap(v)
                                if x == last
                                else read(level - 1, part, k, parity, x + 1, r)
                            )
                            along = read(level - 1, part, k, parity, x - 1, r) + inner
                            across = (
                                read(level - 1, part, k, parity, x, r - 1)
                                + read(level - 1, part, k, parity, x, r + 1)
                            ) + (other + turn(other, 4 if parity == 0 else -4))
                            near.append(
                                (
                                    read(0, part, k, parity, x, r) + (1.0 - relaxation) * v,
                                    (couple_first / couple_cross) * along + across,
                                )
                            )
                        (rest_real, near_real), (rest_imag, near_imag) = near
                        values = (
                            rest_real + (a * near_real + b * near_imag),
                            rest_imag + (c * near_real + d * near_imag),
                        )
                        here = slice(r, r + CHUNK)
                        for part, value in enumerate(values):
                            m = part * half + 2 * k + parity
                            target[m, x - rows.start, here] = value
            return carry

        loop(quarter, 4, mode)

    for key in keys:
        if key[1]:
            sweep(key[1])
    if phase == 0:
        for store in copy_in(sems, [(arrays[key], ref) for key, ref in zip(keys, results)]):
            store.wait()
    if not ends:
        return

    kept = size // 8
    done = [plan.find(phase, SWEEPS - 1, SWEEPS + i) for i in range(pairs)]
    stores = []
    for i, (key, row) in enumerate(done):

        for index in range(kept):
            source = arrays[key]
            r = slice(EDGE + index * 8, EDGE + index * 8 + 8)
            parts = []
            for part in (0, 1):
                values = [None] * half
                for k in range(quarter):
                    even = source[part * half + 2 * k, row, r, :]
                    odd = source[part * half + 2 * k + 1, row, r, :]
                    mask = first_mask(even)
                    values[k] = jnp.where(mask, even, turn(odd, 2))
                    values[k + quarter] = jnp.where(mask, turn(even, -2), odd)
                parts.append(values)
            reals, imags = parts
            modes = [(reals[0], None)] + list(zip(reals[1:], imags[1:])) + [(imags[0], None)]
            for n, value in enumerate(real_inverse(modes)):
                final[n, i, index * 8 : index * 8 + 8] = (1.0 / (horizon * weights[n])) * value
        stores += copy_in(sems.at[pl.ds(i, 1)], [(final.at[:, i], results[0].at[:, i])])
    for store in stores:
        store.wait()


def finish(state, pieces, out, updated, mix, sems):
    count, steps, pairs, size, lanes = pieces.shape
    width = 2 * pairs
    second = lanes // 2
    per = LANES // size
    stores = []
    for step in range(steps):
        for pair in range(pairs):
            mirror = width - 1 - pair
            for part in range(count // per):
                here = slice(part * LANES, (part + 1) * LANES)
                piece = mix.at[pair % 2, part]
                piece[...] = jnp.concatenate(
                    [pieces[part * per + b, step, pair] for b in range(per)], axis=0
                ).T
                low, high = piece[pl.ds(0, second, stride=2), :], piece[pl.ds(1, second, stride=2), :]
                updated[step, pair, :, here] = state[step, pair, :, here] + low
                updated[step, mirror, :, here] = state[step, mirror, :, here] + high
            first = 2 * (step * pairs + pair)
            stores += copy_in(
                sems.at[pl.ds(first, 2)],
                [(updated.at[step, layer], out.at[step, layer]) for layer in (pair, mirror)],
            )
    for store in stores:
        store.wait()


def residual_of(state, carried, lower_hbm, upper_hbm, out, lower, upper, sems):
    steps, width, second, third = state.shape
    parts = third // LANES
    used = pl.ds(0, lower.shape[0])
    loads = copy_in(sems, [(lower_hbm.at[used], lower), (upper_hbm.at[used], upper)])
    for load in loads:
        load.wait()

    def outside(ref, step):
        at = step * parts * second
        return jnp.concatenate(
            [ref[at + part * second : at + (part + 1) * second] for part in range(parts)], axis=1
        )

    for step in range(steps):
        for layer in range(width):
            s = state[step, layer]
            below = outside(lower, step) if layer == 0 else state[step, layer - 1]
            above = outside(upper, step) if layer == width - 1 else state[step, layer + 1]
            before = carried[layer] if step == 0 else state[step - 1, layer]
            across = (
                pltpu.roll(s, 1, 0)
                + pltpu.roll(s, s.shape[0] - 1, 0)
                + pltpu.roll(s, 1, 1)
                + pltpu.roll(s, s.shape[1] - 1, 1)
            )
            centre = time_step - 1.0 - 2.0 * couple_first - 4.0 * couple_cross
            out[step, layer] = (
                (before + couple_first * (below + above))
                + (couple_cross * across + s * (centre - time_step * (s * s)))
            )


def shape_of(*dims):
    return jax.ShapeDtypeStruct(dims, jnp.float32)


def padded_bytes(shape):
    *major, rows, lanes = (1, 1, *shape)
    return 4 * math.prod(major) * (-(-rows // 8) * 8) * (-(-lanes // 128) * 128)


def call(kernel, outs, args, scratch=(), flops=2e6, scalars=0, far=(), far_outs=()):
    spaces = [
        pltpu.SMEM if i < scalars else pltpu.HBM if i in far else pltpu.VMEM for i in range(len(args))
    ]
    out_spaces = [pltpu.HBM if i in far_outs else pltpu.VMEM for i in range(len(outs))]
    held = [a.shape for i, a in enumerate(args) if i not in far]
    held += [o.shape for i, o in enumerate(outs) if i not in far_outs]
    held += [r.shape for r in scratch if len(r.shape) > 1]
    moved = sum(padded_bytes(a.shape) for a in (*args, *outs))
    args = [
        pltpu.with_memory_space_constraint(a, pltpu.HBM) if i in far else a for i, a in enumerate(args)
    ]
    outs = [pltpu.HBM(o.shape, o.dtype) if i in far_outs else o for i, o in enumerate(outs)]
    return pl.pallas_call(
        kernel,
        out_shape=tuple(outs),
        in_specs=[pl.BlockSpec(memory_space=space) for space in spaces],
        out_specs=tuple(pl.BlockSpec(memory_space=space) for space in out_spaces),
        scratch_shapes=list(scratch),
        compiler_params=pltpu.CompilerParams(
            vmem_limit_bytes=sum(padded_bytes(s) for s in held) + 2 * MIB
        ),
        cost_estimate=pl.CostEstimate(
            flops=int(flops), bytes_accessed=int(moved), transcendentals=0
        ),
    )(*args)


def vmem(*shape):
    return pltpu.VMEM(shape, jnp.float32)


def semaphores(count):
    return pltpu.SemaphoreType.DMA((count,))


def exchange(block):
    return lax.all_to_all(block, "tm", split_axis=0, concat_axis=0, tiled=True)


def iteration(state, initial):
    steps, width, second, third = state.shape
    count = lax.axis_size("tm")
    horizon = steps * count
    half = horizon // 2
    position = lax.axis_index("tm")
    pairs = width // 2
    size = third // count
    lanes = 2 * second
    stage = vmem(2, third + 2 * PAD, lanes)
    mixer = vmem(2, third // LANES, lanes, LANES)

    raw_rows = EARLY * steps * second * (third // LANES)
    sent_rows = raw_rows + (SWEEPS // 2) * (size + 2 * SWEEPS - 4)
    own_shape = (count, steps, pairs * (size + 2 * SWEEPS), lanes)
    first_shape = (pairs, size + 2 * PAD, lanes)
    sent, first, up, down = call(
        pack_own,
        [
            shape_of(*own_shape),
            shape_of(*first_shape),
            shape_of(sent_rows, LANES),
            shape_of(sent_rows, LANES),
        ],
        [position.reshape(1), state, initial],
        [
            vmem(*state.shape),
            vmem(*initial.shape),
            vmem(*own_shape),
            vmem(*first_shape),
            vmem(sent_rows - raw_rows, LANES),
            vmem(sent_rows - raw_rows, LANES),
            stage,
            mixer,
            semaphores(4 * pairs),
            semaphores(pairs // 2 + 1),
            semaphores(2 * EARLY * steps * (third // LANES) + 2),
        ],
        scalars=1,
        far=(1, 2),
        far_outs=(0, 1, 2, 3),
    )
    own = exchange(sent).reshape(horizon, -1, lanes)

    lower = hop(up, 1)
    upper = hop(down, -1)

    late_shape = shape_of(half * sum(late_rows(size)), lanes)
    late_up, late_down = call(functools.partial(pack_late, pairs, size), [late_shape] * 2, [own])
    late_low = hop(late_up, 1)
    late_high = hop(late_down, -1)

    early_shape = (count, steps, sum(early_rows(size)), lanes)
    kept = shape_of(steps * second * (third // LANES) + sent_rows - raw_rows, LANES)
    sent_early, kept_low, kept_high = call(
        pack_early,
        [shape_of(*early_shape), kept, kept],
        [late_up, lower, upper],
        [vmem(*early_shape), stage, mixer, semaphores(2 * steps + 2 + SPLIT * steps)],
        far=(0,),
        far_outs=(0, 1, 2),
    )
    early = exchange(sent_early).reshape(horizon, -1, lanes)

    carried = lax.ppermute(state[steps - 1], "tm", [(i, i + 1) for i in range(count - 1)])
    carried = jnp.where(position == 0, initial, carried)
    (residual,) = call(
        residual_of,
        [shape_of(*state.shape)],
        [state, carried, kept_low, kept_high],
        [vmem(raw_rows // EARLY, LANES), vmem(raw_rows // EARLY, LANES), semaphores(2)],
        flops=6e6,
        far=(2, 3),
    )

    plan = Plan(pairs)
    table = jnp.asarray(sweep_table(horizon, lanes))
    arrays = {}
    for phase in range(plan.final + 1):
        ends = phase == plan.final
        inputs = {"table": table, "own": own, "first": first}
        if phase:
            inputs |= {"early": early, "first_low": kept_low, "first_high": kept_high}
        if ends:
            inputs |= {"late_low": late_low, "late_high": late_high}
        inputs |= {key: arrays[key] for key in plan.needed(phase)}
        keys = plan.arrays(phase)
        outs = [shape_of(*plan.shape(key, horizon, size, lanes)) for key in keys]
        fresh = len(plan.fresh(phase))
        halo = vmem((SWEEPS // 2) * (size + 2 * (SWEEPS - 2)), lanes)
        far = [n for n in inputs if n in FAR or n[0] == 0]
        near = [halo if n[:6] == "first_" else vmem(*inputs[n].shape) for n in far]
        scratch = near + [
            vmem(horizon + 1, fresh + 2, size + 2 * EDGE + 2 * PAD, lanes),
            vmem(horizon, fresh, size + 2 * EDGE, lanes),
            semaphores(max(len(far), len(keys), pairs)),
        ]
        inner = [vmem(*o.shape) for o in outs]
        if phase == 0:
            scratch = inner + scratch
        if ends:
            scratch = inner + [vmem(horizon, pairs, size, lanes)] + scratch
            outs = [shape_of(horizon, pairs, size, lanes)]
        results = call(
            functools.partial(solve, phase, plan, pairs, size, list(inputs), far),
            outs,
            list(inputs.values()),
            scratch,
            flops=3e7,
            far=[i for i, n in enumerate(inputs) if n in far],
            far_outs=range(len(outs)) if ends or phase == 0 else (),
        )
        arrays |= {} if ends else dict(zip(keys, results))
    moved = results[0].reshape(count, steps, pairs, size, lanes)

    pieces = exchange(moved)
    (updated,) = call(
        finish,
        [shape_of(*state.shape)],
        [state, pieces],
        [vmem(*state.shape), mixer, semaphores(steps * width)],
        far_outs=(0,),
    )
    return (updated, residual)


def solution(mesh):
    in_specs = (P("tm", "space", None, None), P("space", None, None))
    out_specs = (P("tm", "space", None, None), P("tm", "space", None, None))
    return jax.shard_map(iteration, mesh=mesh, in_specs=in_specs, out_specs=out_specs, check_vma=False)
```

```python
import functools
import math

import jax
import jax.numpy as jnp
import numpy as np
from jax import lax
from jax.experimental import pallas as pl
from jax.experimental.pallas import tpu as pltpu
from jax.sharding import PartitionSpec as P


SWEEPS = 6
EARLY = 3

alpha_value = 0.1
time_step = 0.1
couple_first = 0.4
couple_cross = 0.05
reaction_shift = 0.1
relaxation = 0.9

SPLIT = 4
CHUNK = 8
LANES = 128
PAD = 8
EDGE = 12
MIB = 1024 * 1024


def reach(depth):
    return SWEEPS - max(depth, 0)


def ring(axis, step):
    count = lax.axis_size(axis)
    return [(i, (i + step) % count) for i in range(count)]


def hop(block, step):
    return lax.ppermute(block, "space", ring("space", step))


def low_mask(tile):
    return lax.broadcasted_iota(jnp.int32, tile.shape, tile.ndim - 1) % 2 == 0


def first_mask(tile):
    return lax.broadcasted_iota(jnp.int32, tile.shape, tile.ndim - 1) // 2 % 2 == 0


def turn(tile, step):
    return pltpu.roll(tile, step % tile.shape[-1], tile.ndim - 1)


def merge(low, high, low_at=0, high_at=1):
    low = turn(low, -1) if low_at else low
    high = high if high_at else turn(high, 1)
    return jnp.where(low_mask(low), low, high)


def swap(tile):
    return jnp.where(low_mask(tile), turn(tile, -1), turn(tile, 1))


def stage_tile(mix, stage):
    third = mix.shape[0] * LANES
    for part in range(mix.shape[0]):
        stage[PAD + part * LANES : PAD + (part + 1) * LANES] = mix[part].T
    stage[:PAD] = stage[third : third + PAD]
    stage[third + PAD :] = stage[PAD : 2 * PAD]


def layer_half(layer, width):
    return (layer, True) if 2 * layer < width else (width - 1 - layer, False)


def copy_in(sems, pairs):
    copies = [pltpu.make_async_copy(a, b, sems.at[i]) for i, (a, b) in enumerate(pairs)]
    for copy in copies:
        copy.start()
    return copies


def split(source, target, step):
    some = source.shape[0] // SPLIT
    return [
        (source.at[pl.ds(i * some, some), step], target.at[pl.ds(i * some, some), step])
        for i in range(SPLIT)
    ]


def pack_own(
    position,
    state_hbm,
    initial_hbm,
    out_hbm,
    first_hbm,
    up_hbm,
    down_hbm,
    state,
    initial,
    out,
    first,
    up,
    down,
    stage,
    mix,
    sems,
    out_sems,
    halo_sems,
):
    count, steps = out.shape[:2]
    width, second, third = state.shape[1:]
    size = third // count
    pairs = width // 2
    rows = size + 2 * SWEEPS
    parts = third // LANES
    loads = []
    for pair in range(pairs):
        for i, layer in enumerate((pair, width - 1 - pair)):
            loads += copy_in(
                sems.at[pl.ds(4 * pair + 2 * i, 2)],
                [(state_hbm.at[:, layer], state.at[:, layer]), (initial_hbm.at[layer], initial.at[layer])],
            )
    stores = []
    for pair in range(pairs):
        for load in loads[4 * pair : 4 * pair + 4]:
            load.wait()
        if pair < EARLY:
            pieces = []
            for step in range(steps):
                for part in range(parts):
                    here = pl.ds(part * LANES, LANES)
                    for target, layer, j in (
                        (up_hbm, width - 1 - pair, EARLY - 1 - pair),
                        (down_hbm, pair, pair),
                    ):
                        row = ((step * EARLY + j) * parts + part) * second
                        pieces.append((state.at[step, layer, :, here], target.at[pl.ds(row, second)]))
            stores += copy_in(halo_sems.at[pl.ds(pair * len(pieces), len(pieces))], pieces)
        for step in range(steps + 1):
            slot = step % 2
            for part in range(parts):
                here = slice(part * LANES, (part + 1) * LANES)
                for half, layer in enumerate((pair, width - 1 - pair)):
                    source = state[step, layer, :, here] if step < steps else initial[layer, :, here]
                    mix[slot, part, pl.ds(half, second, stride=2), :] = source
            stage_tile(mix.at[slot], stage.at[slot])
            if step < steps:
                for b in range(count):
                    begin = PAD - SWEEPS + b * size
                    out[b, step, pair * rows : (pair + 1) * rows] = stage[slot, begin : begin + rows]
            else:
                begin = pl.multiple_of(position[0] * size, 8)
                first[pair] = stage[slot, pl.ds(begin, size + 2 * PAD), :]
        if pair % 2:
            here = pl.ds((pair - 1) * rows, 2 * rows)
            stores += copy_in(
                out_sems.at[pl.ds(pair // 2, 1)],
                [(out.at[:, :, here], out_hbm.at[:, :, here])],
            )
    stores += copy_in(out_sems.at[pl.ds(pairs // 2, 1)], [(first, first_hbm)])
    at = 0
    short = size + 2 * (SWEEPS - 2)
    begin = PAD - SWEEPS + 2
    for slot in range(SWEEPS // 2):
        for out_ref, layers in (
            (up, [width - a for a in (2 * slot + 1, 2 * slot + 2)]),
            (down, [a - 1 for a in (2 * slot + 1, 2 * slot + 2)]),
        ):
            (one, one_low), (two, two_low) = [layer_half(layer, width) for layer in layers]
            out_ref[at : at + short] = merge(
                first[one, begin : begin + short],
                first[two, begin : begin + short],
                0 if one_low else 1,
                0 if two_low else 1,
            )
        at += short
    raw = up_hbm.shape[0] - at
    stores += copy_in(
        halo_sems.at[pl.ds(2 * EARLY * steps * parts, 2)],
        [(up, up_hbm.at[pl.ds(raw, at)]), (down, down_hbm.at[pl.ds(raw, at)])],
    )
    for store in stores:
        store.wait()


def early_rows(size):
    return [size + 2 * reach(EARLY - j) for j in range(EARLY)]


def late_rows(size):
    return [size + 2 * reach(SWEEPS - j) for j in range(SWEEPS - EARLY)]


def offsets(sizes):
    return [sum(sizes[:i]) for i in range(len(sizes))]


def pack_early(after, lower, upper, out_hbm, kept_low, kept_high, out, stage, mix, sems):
    count, steps = out.shape[:2]
    parts = mix.shape[1]
    second = mix.shape[2] // 2
    size = parts * LANES // count
    sizes = early_rows(size)
    layer = parts * second
    raw = EARLY * steps * layer
    stores = []
    for i, (source, target, nearest) in enumerate(
        ((lower, kept_low, EARLY - 1), (upper, kept_high, 0))
    ):
        pieces = [
            (source.at[pl.ds((step * EARLY + nearest) * layer, layer)], target.at[pl.ds(step * layer, layer)])
            for step in range(steps)
        ]
        rest = source.shape[0] - raw
        pieces.append((source.at[pl.ds(raw, rest)], target.at[pl.ds(steps * layer, rest)]))
        stores += copy_in(sems.at[pl.ds(i * (steps + 1), steps + 1)], pieces)
    for step in range(steps):
        for j, (rows, at) in enumerate(zip(sizes, offsets(sizes))):
            slot = j % 2
            for part in range(parts):
                low = ((step * EARLY + j) * parts + part) * second
                high = ((step * EARLY + EARLY - 1 - j) * parts + part) * second
                mix[slot, part, pl.ds(0, second, stride=2), :] = lower[low : low + second]
                mix[slot, part, pl.ds(1, second, stride=2), :] = upper[high : high + second]
            stage_tile(mix.at[slot], stage.at[slot])
            for b in range(count):
                begin = PAD - (rows - size) // 2 + b * size
                out[b, step, at : at + rows] = stage[slot, begin : begin + rows]
        stores += copy_in(
            sems.at[pl.ds(2 * steps + 2 + step * SPLIT, SPLIT)], split(out, out_hbm, step)
        )
    for store in stores:
        store.wait()


def pack_late(pairs, size, own, up_hbm, down_hbm, up, down, sems):
    horizon = own.shape[0]
    half = horizon // 2
    width = 2 * pairs
    stride = size + 2 * SWEEPS
    at = 0
    stores = []
    for j, rows in enumerate(late_rows(size)):
        a = SWEEPS - j
        for t in range(half):
            for out, layer in ((up, width - a), (down, a - 1)):
                pair, low = layer_half(layer, width)
                begin = pair * stride + (stride - rows) // 2
                before = own[t, begin : begin + rows]
                after = own[t + half, begin : begin + rows]
                here = 0 if low else 1
                out[at : at + rows] = merge(before, after, here, here)
            at += rows
        region = pl.ds(at - half * rows, half * rows)
        stores += copy_in(
            sems.at[pl.ds(2 * j, 2)],
            [(up.at[region], up_hbm.at[region]), (down.at[region], down_hbm.at[region])],
        )
    for store in stores:
        store.wait()


def real_forward(values):
    count = len(values)
    if count == 1:
        return [(values[0], None)]
    if count == 2:
        return [(values[0] + values[1], None), (values[0] - values[1], None)]
    even = real_forward(values[0::2])
    odd = real_forward(values[1::2])
    half = count // 2
    result = [None] * (half + 1)
    for k in range(count // 4 + 1):
        even_real, even_imag = even[k]
        odd_real, odd_imag = odd[k]
        if k == 0:
            result[0] = (even_real + odd_real, None)
            result[half] = (even_real - odd_real, None)
        elif 4 * k == count:
            result[k] = (even_real, -odd_real)
        else:
            cos, sin = math.cos(2 * math.pi * k / count), math.sin(2 * math.pi * k / count)
            if odd_imag is None:
                turned_real, turned_imag = cos * odd_real, -sin * odd_real
            else:
                turned_real = cos * odd_real + sin * odd_imag
                turned_imag = cos * odd_imag - sin * odd_real
            if even_imag is None:
                result[k] = (even_real + turned_real, turned_imag)
                result[half - k] = (even_real - turned_real, turned_imag)
            else:
                result[k] = (even_real + turned_real, even_imag + turned_imag)
                result[half - k] = (even_real - turned_real, turned_imag - even_imag)
    return result


def real_inverse(modes):
    half = len(modes) - 1
    count = 2 * half
    if count == 2:
        return [modes[0][0] + modes[1][0], modes[0][0] - modes[1][0]]
    even, odd = [], []
    for k in range(count // 4 + 1):
        real, imag = modes[k]
        other_real, other_imag = modes[half - k]
        if k == 0:
            even.append((real + other_real, None))
            odd.append((real - other_real, None))
        elif 4 * k == count:
            even.append((2.0 * real, None))
            odd.append((-2.0 * imag, None))
        else:
            cos, sin = math.cos(2 * math.pi * k / count), math.sin(2 * math.pi * k / count)
            even.append((real + other_real, imag - other_imag))
            minus_real, minus_imag = real - other_real, imag + other_imag
            odd.append((cos * minus_real - sin * minus_imag, sin * minus_real + cos * minus_imag))
    result = [None] * count
    result[0::2] = real_inverse(even)
    result[1::2] = real_inverse(odd)
    return result


def mode_inverses(horizon):
    rho = alpha_value ** (1.0 / horizon)
    angles = 2.0 * math.pi * np.arange(horizon // 2 + 1) / horizon
    shift = (
        1.0 + reaction_shift + 2.0 * couple_first + 4.0 * couple_cross - rho * np.cos(angles)
    ) + 1j * rho * np.sin(angles)
    return 1.0 / shift


def sweep_table(horizon, lanes):
    inverse = relaxation * mode_inverses(horizon)
    rows = [(inverse[0].real, 0.0, 0.0, inverse[-1].real)]
    rows += [(v.real, -v.imag, v.imag, v.real) for v in inverse[1:-1]]
    table = couple_cross * np.array(rows)
    quarter = horizon // 4
    mode = np.arange(quarter)[:, None] + quarter * (np.arange(lanes) // 2 % 2)[None, :]
    spread = np.moveaxis(table[mode], -1, 1)[:, :, None, :]
    return np.broadcast_to(spread, (quarter, 4, 8, lanes)).astype(np.float32)


FAR = ("late_low", "late_high", "first", "first_low", "first_high")


class Plan:
    def __init__(self, pairs):
        self.last = SWEEPS + pairs - 1
        self.begins = [SWEEPS, 0]
        self.final = len(self.begins) - 1

    def fresh(self, phase):
        end = self.last if phase == 0 else self.begins[phase - 1]
        return range(self.begins[phase] + 1, end + 1)

    def rows(self, phase, level):
        fresh = self.fresh(phase)
        return range(fresh.start + level, min(fresh.stop - 1 + level, self.last) + 1)

    def arrays(self, phase):
        return [(phase, level) for level in range(SWEEPS) if self.rows(phase, level)]

    def find(self, phase, level, row):
        for p in range(phase, -1, -1):
            if row in self.rows(p, level):
                return (p, level), row - self.rows(p, level).start
        raise ValueError((phase, level, row))

    def needed(self, phase):
        keys = set()
        for level in range(1, SWEEPS):
            for row in self.rows(phase, level):
                keys.add(self.find(phase, 0, row)[0])
                for x in (row - 1, row, min(row + 1, self.last)):
                    keys.add(self.find(phase, level - 1, x)[0])
        if phase == self.final:
            for row in range(SWEEPS, self.last + 1):
                keys.add(self.find(phase, SWEEPS - 1, row)[0])
        return sorted(k for k in keys if k[0] < phase)

    def shape(self, key, horizon, size, lanes):
        rows = size + 2 * EDGE
        return (horizon, len(self.rows(*key)), rows, lanes)


def loop(count, copies, step):
    while count % copies:
        copies -= 1

    def several(index, carry):
        for i in range(copies):
            step(index * copies + i, 0)
        return carry

    lax.fori_loop(0, count // copies, several, 0)


def second_sum(tile):
    return turn(tile, 2) + turn(tile, -2)


def solve(phase, plan, pairs, size, names, far, *refs):
    named = dict(zip(names, refs))
    outs = refs[len(names) :]
    state, weighted, sems = refs[-3:]
    near = refs[-3 - len(far) : -3]
    halo = (SWEEPS // 2) * (size + 2 * (SWEEPS - 2))
    sources = {}
    for name in far:
        sources[name] = named[name]
        if name in ("first_low", "first_high"):
            sources[name] = named[name].at[pl.ds(named[name].shape[0] - halo, halo)]
    loads = dict(zip(far, copy_in(sems, [(sources[n], r) for n, r in zip(far, near)])))
    named |= dict(zip(far, near))
    horizon = weighted.shape[0]
    half, quarter = horizon // 2, horizon // 4
    last = plan.last
    window = size + 2 * EDGE
    at = PAD
    fresh = plan.fresh(phase)
    held = range(fresh.start - 1, fresh.stop + 1)
    keys = plan.arrays(phase)
    count = len(keys)
    ends = phase == plan.final
    results = outs[:1] if ends else outs[:count]
    inner_refs = refs[len(names) + len(results) :][:count] if ends or phase == 0 else results
    final = refs[len(names) + 1 + count] if ends else None
    arrays = dict(zip(keys, inner_refs))
    for key in plan.needed(phase):
        arrays[key] = named[key]

    own, early, first = named["own"], named.get("early"), named["first"]
    early_sizes, late_sizes = early_rows(size), late_rows(size)
    early_at, late_at = offsets(early_sizes), offsets([half * rows for rows in late_sizes])
    late_count = SWEEPS - EARLY
    own_rows = size + 2 * SWEEPS

    def fill(t, carry):
        for x in held:
            if x > last:
                continue
            if x >= SWEEPS:
                begin = at + EDGE - SWEEPS
                state[1 + t, x - held.start, begin : begin + own_rows] = own[
                    t, (x - SWEEPS) * own_rows : (x - SWEEPS + 1) * own_rows
                ]
            elif x >= late_count:
                j = x - late_count
                begin = at + EDGE - (early_sizes[j] - size) // 2
                state[1 + t, x - held.start, begin : begin + early_sizes[j]] = early[
                    t, early_at[j] : early_at[j] + early_sizes[j]
                ]
        return carry

    loop(horizon, 4, fill)
    for name in FAR:
        if name in loads:
            loads.pop(name).wait()
    for x in held:
        if x < late_count:
            rows, where = late_sizes[x], late_at[x]
            begin = at + EDGE - (rows - size) // 2
            for t in range(half):
                low = named["late_low"][where + t * rows : where + (t + 1) * rows]
                high = named["late_high"][where + t * rows : where + (t + 1) * rows]
                state[1 + t, x - held.start, begin : begin + rows] = merge(low, high, 0, 0)
                state[1 + half + t, x - held.start, begin : begin + rows] = merge(low, high, 1, 1)
    for x in fresh:
        if x >= SWEEPS:
            begin = at + EDGE - PAD
            state[0, x - held.start, begin : begin + size + 2 * PAD] = first[x - SWEEPS]
        else:
            a = SWEEPS - x
            rows = size + 2 * (SWEEPS - 2)
            total = named["first_low"].shape[0]
            where = total - (SWEEPS // 2 - (a - 1) // 2) * rows
            low, high = named["first_low"][where : where + rows], named["first_high"][where : where + rows]
            slot = (a - 1) % 2
            tile = merge(low, high, slot, slot)
            begin = at + EDGE - SWEEPS + 2
            state[0, x - held.start, begin : begin + rows] = tile

    def weigh(t, carry):
        centre = time_step - 1.0 - 2.0 * couple_first - 4.0 * couple_cross
        for i in range(len(fresh)):
            for r in range(at, at + window, CHUNK):
                s = state[t + 1, i + 1, r : r + CHUNK]
                outer = state[t + 1, i, r : r + CHUNK]
                along = outer + (swap(s) if fresh[i] == last else state[t + 1, i + 2, r : r + CHUNK])
                across = (
                    state[t + 1, i + 1, r - 1 : r + CHUNK - 1]
                    + state[t + 1, i + 1, r + 1 : r + CHUNK + 1]
                    + second_sum(s)
                )
                weighted[t, i, r - at : r - at + CHUNK] = (
                    (state[t, i + 1, r : r + CHUNK] + couple_first * along)
                    + (couple_cross * across + s * (centre - time_step * (s * s)))
                )
        return carry

    loop(horizon, 8, weigh)

    inverses = mode_inverses(horizon)
    weights = [alpha_value ** (n / horizon) for n in range(horizon)]
    tiles = window // 8
    base = arrays[(phase, 0)]

    def transform(index, carry):
        i = index // tiles
        r = pl.ds(pl.multiple_of((index % tiles) * 8, 8), 8)
        spectrum = real_forward([weights[n] * weighted[n, i, r, :] for n in range(horizon)])
        reals, imags = [None] * half, [None] * half
        for k, (real, imag) in enumerate(spectrum):
            c = relaxation * inverses[k]
            if k == 0:
                reals[0] = float(c.real) * real
            elif k == half:
                imags[0] = float(c.real) * real
            else:
                reals[k] = float(c.real) * real - float(c.imag) * imag
                imags[k] = float(c.imag) * real + float(c.real) * imag
        for part, values in enumerate((reals, imags)):
            for k in range(quarter):
                one, two = values[k], values[k + quarter]
                mask = first_mask(one)
                base[part * half + 2 * k, i, r, :] = jnp.where(mask, one, turn(two, 2))
                base[part * half + 2 * k + 1, i, r, :] = jnp.where(mask, turn(one, -2), two)
        return carry

    loop(len(fresh) * tiles, 7, transform)

    table = named["table"]
    for load in loads.values():
        load.wait()

    def sweep(level):
        rows = plan.rows(phase, level)
        span = size + PAD
        begin = EDGE - PAD // 2
        target = arrays[(phase, level)]

        def read(level_, part, k, parity, x, r):
            key, i = plan.find(phase, level_, x)
            return arrays[key][part * half + 2 * k + parity, i, r : r + CHUNK]

        def mode(k, carry):
            a, b, c, d = [table[k, i] for i in range(4)]
            for x in rows:
                for r in range(begin, begin + span, CHUNK):
                    for parity in (0, 1):
                        near = []
                        for part in (0, 1):
                            v = read(level - 1, part, k, parity, x, r)
                            other = read(level - 1, part, k, 1 - parity, x, r)
                            inner = (
                                swap(v)
                                if x == last
                                else read(level - 1, part, k, parity, x + 1, r)
                            )
                            along = read(level - 1, part, k, parity, x - 1, r) + inner
                            across = (
                                read(level - 1, part, k, parity, x, r - 1)
                                + read(level - 1, part, k, parity, x, r + 1)
                            ) + (other + turn(other, 4 if parity == 0 else -4))
                            near.append(
                                (
                                    read(0, part, k, parity, x, r) + (1.0 - relaxation) * v,
                                    (couple_first / couple_cross) * along + across,
                                )
                            )
                        (rest_real, near_real), (rest_imag, near_imag) = near
                        values = (
                            rest_real + (a * near_real + b * near_imag),
                            rest_imag + (c * near_real + d * near_imag),
                        )
                        here = slice(r, r + CHUNK)
                        for part, value in enumerate(values):
                            m = part * half + 2 * k + parity
                            target[m, x - rows.start, here] = value
            return carry

        loop(quarter, 4, mode)

    for key in keys:
        if key[1]:
            sweep(key[1])
    if phase == 0:
        for store in copy_in(sems, [(arrays[key], ref) for key, ref in zip(keys, results)]):
            store.wait()
    if not ends:
        return

    kept = size // 8
    done = [plan.find(phase, SWEEPS - 1, SWEEPS + i) for i in range(pairs)]
    stores = []
    for i, (key, row) in enumerate(done):

        for index in range(kept):
            source = arrays[key]
            r = slice(EDGE + index * 8, EDGE + index * 8 + 8)
            parts = []
            for part in (0, 1):
                values = [None] * half
                for k in range(quarter):
                    even = source[part * half + 2 * k, row, r, :]
                    odd = source[part * half + 2 * k + 1, row, r, :]
                    mask = first_mask(even)
                    values[k] = jnp.where(mask, even, turn(odd, 2))
                    values[k + quarter] = jnp.where(mask, turn(even, -2), odd)
                parts.append(values)
            reals, imags = parts
            modes = [(reals[0], None)] + list(zip(reals[1:], imags[1:])) + [(imags[0], None)]
            for n, value in enumerate(real_inverse(modes)):
                final[n, i, index * 8 : index * 8 + 8] = (1.0 / (horizon * weights[n])) * value
        stores += copy_in(sems.at[pl.ds(i, 1)], [(final.at[:, i], results[0].at[:, i])])
    for store in stores:
        store.wait()


def finish(state, pieces, out, updated, mix, sems):
    count, steps, pairs, size, lanes = pieces.shape
    width = 2 * pairs
    second = lanes // 2
    per = LANES // size
    stores = []
    for step in range(steps):
        for pair in range(pairs):
            mirror = width - 1 - pair
            for part in range(count // per):
                here = slice(part * LANES, (part + 1) * LANES)
                piece = mix.at[pair % 2, part]
                piece[...] = jnp.concatenate(
                    [pieces[part * per + b, step, pair] for b in range(per)], axis=0
                ).T
                low, high = piece[pl.ds(0, second, stride=2), :], piece[pl.ds(1, second, stride=2), :]
                updated[step, pair, :, here] = state[step, pair, :, here] + low
                updated[step, mirror, :, here] = state[step, mirror, :, here] + high
            first = 2 * (step * pairs + pair)
            stores += copy_in(
                sems.at[pl.ds(first, 2)],
                [(updated.at[step, layer], out.at[step, layer]) for layer in (pair, mirror)],
            )
    for store in stores:
        store.wait()


def residual_of(state, carried, lower_hbm, upper_hbm, out, lower, upper, sems):
    steps, width, second, third = state.shape
    parts = third // LANES
    used = pl.ds(0, lower.shape[0])
    loads = copy_in(sems, [(lower_hbm.at[used], lower), (upper_hbm.at[used], upper)])
    for load in loads:
        load.wait()

    def outside(ref, step):
        at = step * parts * second
        return jnp.concatenate(
            [ref[at + part * second : at + (part + 1) * second] for part in range(parts)], axis=1
        )

    for step in range(steps):
        for layer in range(width):
            s = state[step, layer]
            below = outside(lower, step) if layer == 0 else state[step, layer - 1]
            above = outside(upper, step) if layer == width - 1 else state[step, layer + 1]
            before = carried[layer] if step == 0 else state[step - 1, layer]
            across = (
                pltpu.roll(s, 1, 0)
                + pltpu.roll(s, s.shape[0] - 1, 0)
                + pltpu.roll(s, 1, 1)
                + pltpu.roll(s, s.shape[1] - 1, 1)
            )
            centre = time_step - 1.0 - 2.0 * couple_first - 4.0 * couple_cross
            out[step, layer] = (
                (before + couple_first * (below + above))
                + (couple_cross * across + s * (centre - time_step * (s * s)))
            )


def shape_of(*dims):
    return jax.ShapeDtypeStruct(dims, jnp.float32)


def padded_bytes(shape):
    *major, rows, lanes = (1, 1, *shape)
    return 4 * math.prod(major) * (-(-rows // 8) * 8) * (-(-lanes // 128) * 128)


def call(kernel, outs, args, scratch=(), flops=2e6, scalars=0, far=(), far_outs=()):
    spaces = [
        pltpu.SMEM if i < scalars else pltpu.HBM if i in far else pltpu.VMEM for i in range(len(args))
    ]
    out_spaces = [pltpu.HBM if i in far_outs else pltpu.VMEM for i in range(len(outs))]
    held = [a.shape for i, a in enumerate(args) if i not in far]
    held += [o.shape for i, o in enumerate(outs) if i not in far_outs]
    held += [r.shape for r in scratch if len(r.shape) > 1]
    moved = sum(padded_bytes(a.shape) for a in (*args, *outs))
    args = [
        pltpu.with_memory_space_constraint(a, pltpu.HBM) if i in far else a for i, a in enumerate(args)
    ]
    outs = [pltpu.HBM(o.shape, o.dtype) if i in far_outs else o for i, o in enumerate(outs)]
    return pl.pallas_call(
        kernel,
        out_shape=tuple(outs),
        in_specs=[pl.BlockSpec(memory_space=space) for space in spaces],
        out_specs=tuple(pl.BlockSpec(memory_space=space) for space in out_spaces),
        scratch_shapes=list(scratch),
        compiler_params=pltpu.CompilerParams(
            vmem_limit_bytes=sum(padded_bytes(s) for s in held) + 2 * MIB
        ),
        cost_estimate=pl.CostEstimate(
            flops=int(flops), bytes_accessed=int(moved), transcendentals=0
        ),
    )(*args)


def vmem(*shape):
    return pltpu.VMEM(shape, jnp.float32)


def semaphores(count):
    return pltpu.SemaphoreType.DMA((count,))


def exchange(block):
    return lax.all_to_all(block, "tm", split_axis=0, concat_axis=0, tiled=True)


def iteration(state, initial):
    steps, width, second, third = state.shape
    count = lax.axis_size("tm")
    horizon = steps * count
    half = horizon // 2
    position = lax.axis_index("tm")
    pairs = width // 2
    size = third // count
    lanes = 2 * second
    stage = vmem(2, third + 2 * PAD, lanes)
    mixer = vmem(2, third // LANES, lanes, LANES)

    raw_rows = EARLY * steps * second * (third // LANES)
    sent_rows = raw_rows + (SWEEPS // 2) * (size + 2 * SWEEPS - 4)
    own_shape = (count, steps, pairs * (size + 2 * SWEEPS), lanes)
    first_shape = (pairs, size + 2 * PAD, lanes)
    sent, first, up, down = call(
        pack_own,
        [
            shape_of(*own_shape),
            shape_of(*first_shape),
            shape_of(sent_rows, LANES),
            shape_of(sent_rows, LANES),
        ],
        [position.reshape(1), state, initial],
        [
            vmem(*state.shape),
            vmem(*initial.shape),
            vmem(*own_shape),
            vmem(*first_shape),
            vmem(sent_rows - raw_rows, LANES),
            vmem(sent_rows - raw_rows, LANES),
            stage,
            mixer,
            semaphores(4 * pairs),
            semaphores(pairs // 2 + 1),
            semaphores(2 * EARLY * steps * (third // LANES) + 2),
        ],
        scalars=1,
        far=(1, 2),
        far_outs=(0, 1, 2, 3),
    )
    own = exchange(sent).reshape(horizon, -1, lanes)

    lower = hop(up, 1)
    upper = hop(down, -1)

    late_shape = shape_of(half * sum(late_rows(size)), lanes)
    late_up, late_down = call(
        functools.partial(pack_late, pairs, size),
        [late_shape] * 2,
        [own],
        [vmem(*late_shape.shape), vmem(*late_shape.shape), semaphores(2 * (SWEEPS - EARLY))],
        far_outs=(0, 1),
    )
    late_low = hop(late_up, 1)
    late_high = hop(late_down, -1)

    early_shape = (count, steps, sum(early_rows(size)), lanes)
    kept = shape_of(steps * second * (third // LANES) + sent_rows - raw_rows, LANES)
    sent_early, kept_low, kept_high = call(
        pack_early,
        [shape_of(*early_shape), kept, kept],
        [late_up, lower, upper],
        [vmem(*early_shape), stage, mixer, semaphores(2 * steps + 2 + SPLIT * steps)],
        far=(0,),
        far_outs=(0, 1, 2),
    )
    early = exchange(sent_early).reshape(horizon, -1, lanes)

    carried = lax.ppermute(state[steps - 1], "tm", [(i, i + 1) for i in range(count - 1)])
    carried = jnp.where(position == 0, initial, carried)
    (residual,) = call(
        residual_of,
        [shape_of(*state.shape)],
        [state, carried, kept_low, kept_high],
        [vmem(raw_rows // EARLY, LANES), vmem(raw_rows // EARLY, LANES), semaphores(2)],
        flops=6e6,
        far=(2, 3),
    )

    plan = Plan(pairs)
    table = jnp.asarray(sweep_table(horizon, lanes))
    arrays = {}
    for phase in range(plan.final + 1):
        ends = phase == plan.final
        inputs = {"table": table, "own": own, "first": first}
        if phase:
            inputs |= {"early": early, "first_low": kept_low, "first_high": kept_high}
        if ends:
            inputs |= {"late_low": late_low, "late_high": late_high}
        inputs |= {key: arrays[key] for key in plan.needed(phase)}
        keys = plan.arrays(phase)
        outs = [shape_of(*plan.shape(key, horizon, size, lanes)) for key in keys]
        fresh = len(plan.fresh(phase))
        halo = vmem((SWEEPS // 2) * (size + 2 * (SWEEPS - 2)), lanes)
        far = [n for n in inputs if n in FAR or n[0] == 0]
        near = [halo if n[:6] == "first_" else vmem(*inputs[n].shape) for n in far]
        scratch = near + [
            vmem(horizon + 1, fresh + 2, size + 2 * EDGE + 2 * PAD, lanes),
            vmem(horizon, fresh, size + 2 * EDGE, lanes),
            semaphores(max(len(far), len(keys), pairs)),
        ]
        inner = [vmem(*o.shape) for o in outs]
        if phase == 0:
            scratch = inner + scratch
        if ends:
            scratch = inner + [vmem(horizon, pairs, size, lanes)] + scratch
            outs = [shape_of(horizon, pairs, size, lanes)]
        results = call(
            functools.partial(solve, phase, plan, pairs, size, list(inputs), far),
            outs,
            list(inputs.values()),
            scratch,
            flops=3e7,
            far=[i for i, n in enumerate(inputs) if n in far],
            far_outs=range(len(outs)) if ends or phase == 0 else (),
        )
        arrays |= {} if ends else dict(zip(keys, results))
    moved = results[0].reshape(count, steps, pairs, size, lanes)

    pieces = exchange(moved)
    (updated,) = call(
        finish,
        [shape_of(*state.shape)],
        [state, pieces],
        [vmem(*state.shape), mixer, semaphores(steps * width)],
        far_outs=(0,),
    )
    return (updated, residual)


def solution(mesh):
    in_specs = (P("tm", "space", None, None), P("space", None, None))
    out_specs = (P("tm", "space", None, None), P("tm", "space", None, None))
    return jax.shard_map(iteration, mesh=mesh, in_specs=in_specs, out_specs=out_specs, check_vma=False)
```
